256 devices in a mesh: pb: 8 (over z_hi, x), col: 32 (over y, z_lo, core).
Axes of the slice: x: 4, y: 4, z: 8 (z_hi: 2, z_lo: 4; z = z_hi * 4 + z_lo), core: 2. Of those that a mesh axis runs over, the one named last changes fastest.
Arguments:
- queries: bfloat16 [16384, 1024], P(('pb', 'col')), may hold values from -64 to 64
- candidates: bfloat16 [32768, 1024], P(('col', 'pb')), may hold values from -5 to 5
- grades: int32 [16384, 32768], P('pb', 'col'), may hold values from 0 to 4
- query_weights: float32 [16384], P('pb'), may hold values from -0.03125 to 0.03125
Outputs:
- losses: float32 [16384], P('pb')
- query_grad: bfloat16 [16384, 1024], P(('pb', 'col'))
- cand_grad: bfloat16 [32768, 1024], P(('col', 'pb'))
The draws below stay inside these ranges and needn't reach their ends.
All inputs are finite; a program needn't handle non-finite values.
Results may differ from the reference program's by a relative error of at most 0.0071.
Values may be sent and summed in bfloat16 or wider, within the bound.
A program may use at most 128 MiB of HBM per device.

```python
import math
import jax
import jax.numpy as jnp
from jax import lax

D = 1024
GRADES = 5
NQ = 16384
NC = 32768


def embed_pair(key):
    query_key = jax.random.fold_in(key, 11)
    cand_key = jax.random.fold_in(key, 12)
    candidates = jnp.clip(jax.random.normal(cand_key, (NC, D), jnp.float32), -5.0, 5.0)
    queries = jnp.clip(jax.random.normal(query_key, (NQ, D), jnp.float32), -5.0, 5.0)
    return (queries, candidates)


def draw_queries(key, part):
    queries, candidates = embed_pair(key)
    return queries.astype(jnp.bfloat16)


def draw_candidates(key, part):
    queries, candidates = embed_pair(key)
    return candidates.astype(jnp.bfloat16)


def draw_grades(key, part):
    kind_key = jax.random.fold_in(key, 21)
    single_key = jax.random.fold_in(key, 22)
    cell_key = jax.random.fold_in(key, 23)
    kinds = jax.random.randint(kind_key, (NQ, 1), 0, 16)
    single = jax.random.randint(single_key, (NQ, 1), 0, GRADES)
    cells = jax.random.randint(cell_key, (NQ, NC), 0, 60)
    spread = cells % GRADES
    upper = 1 + cells % 4
    middle = 2 + cells % 2
    lower = cells % 3
    grades = jnp.where(kinds == 0, upper, jnp.where(kinds == 1, middle, jnp.where(kinds == 2, single, jnp.where(kinds == 3, lower, spread))))
    return grades.astype(jnp.int32)


def steps_of(key, dims, split, smallest, high):
    factor_of, own = 1.0, jax.random.fold_in(key, 6)
    for position, shards_of in split:
        heights = jnp.exp(jax.random.uniform(jax.random.fold_in(own, position), (shards_of,), jnp.float32, smallest / len(split), high / len(split)))
        factor_of = factor_of * jnp.repeat(heights, dims[position] // shards_of).reshape([-1 if axis == position else 1 for axis in range(len(dims))])
    return factor_of


def noise(rng, dims, scale, limit, split=(), held_as=jnp.bfloat16):
    result = scale * jax.random.normal(rng, dims, jnp.float32)
    if split:
        result = result * steps_of(rng, dims, split, -0.22, 0.18)
    return jnp.clip(result, -limit, limit).astype(held_as)


def setup_inputs(seed: int = 0) -> dict:
    streams_of = jax.random.split(jax.random.key(seed), 5)
    return {
        "queries": draw_queries(jax.random.fold_in(streams_of[4], 71), 0),
        "candidates": draw_candidates(jax.random.fold_in(streams_of[4], 71), 0),
        "grades": draw_grades(jax.random.fold_in(streams_of[4], 71), 0),
        "query_weights": noise(streams_of[3], (NQ,), NC ** -0.5, 0.03125, ((0, 8),), jnp.float32),
    }


lowest = -1e+30

def grade_levels(maxima, masses, counts):
    levels = []
    running = maxima[0]
    seen_count = counts[0] * 0.0
    for bucket in range(len(maxima)):
        running = jnp.maximum(running, maxima[bucket])
        seen_count = seen_count + counts[bucket]
        summed = masses[0] * jnp.exp(maxima[0] - running)
        for lesser in range(1, bucket + 1):
            summed = summed + masses[lesser] * jnp.exp(maxima[lesser] - running)
        present = seen_count > 0.0
        levels.append(jnp.where(present, running + jnp.log(jnp.where(present, summed, 1.0)), running))
    return levels

def slope_factors(maxima, levels, counts):
    factors = []
    for bucket in range(len(maxima)):
        summed = counts[bucket] * jnp.exp(maxima[bucket] - levels[bucket])
        for higher in range(bucket + 1, len(maxima)):
            summed = summed + counts[higher] * jnp.exp(maxima[bucket] - levels[higher])
        factors.append(summed)
    return factors

def block_terms(scores, grade_block, weights):
    maxima, masses, counts = ([], [], [])
    for bucket in range(GRADES):
        member = grade_block == bucket
        highest = lax.optimization_barrier(jnp.max(jnp.where(member, scores, lowest), axis=1))
        masses.append(lax.optimization_barrier(jnp.sum(jnp.exp(jnp.where(member, scores - highest[:, None], lowest)), axis=1)))
        counts.append(lax.optimization_barrier(jnp.sum(member.astype(jnp.float32), axis=1)))
        maxima.append(highest)
    totals = lax.optimization_barrier(jnp.sum(scores, axis=1))
    levels = grade_levels(maxima, masses, counts)
    weighted = counts[0] * levels[0]
    for bucket in range(1, GRADES):
        weighted = weighted + counts[bucket] * levels[bucket]
    losses = (weighted - totals) / NC
    factors = slope_factors(maxima, levels, counts)
    picked_factor = jnp.zeros(scores.shape, jnp.float32)
    picked_max = jnp.zeros(scores.shape, jnp.float32)
    for bucket in range(GRADES):
        member = grade_block == bucket
        picked_factor = jnp.where(member, factors[bucket][:, None], picked_factor)
        picked_max = jnp.where(member, maxima[bucket][:, None], picked_max)
    slopes = (weights[:, None] * (picked_factor * jnp.exp(scores - picked_max) - 1.0)).astype(jnp.bfloat16)
    return (losses, slopes)

def reference(queries, candidates, grades, query_weights):
    scaling = 1.0 / math.sqrt(D)
    block_rows = math.gcd(NQ, 256)
    blocks = NQ // block_rows
    query_blocks = queries.reshape(blocks, block_rows, D)
    grade_blocks = grades.reshape(blocks, block_rows, NC)
    weight_blocks = query_weights.reshape(blocks, block_rows)

    def advance(cand_total, pieces):
        row_block, grade_block, weights = pieces
        scores = jnp.dot(row_block, candidates.T, preferred_element_type=jnp.float32) * scaling
        losses, slopes = block_terms(scores, grade_block, weights)
        query_part = (jnp.dot(slopes, candidates, preferred_element_type=jnp.float32) * scaling).astype(jnp.bfloat16)
        cand_total = cand_total + lax.dot_general(slopes, row_block, (((0,), (0,)), ((), ())), preferred_element_type=jnp.float32)
        return (cand_total, (losses, query_part))
    initial = jnp.zeros((NC, D), jnp.float32)
    final, (losses, query_parts) = lax.scan(advance, initial, (query_blocks, grade_blocks, weight_blocks))
    return (losses.reshape(NQ), query_parts.reshape(NQ, D), (final * scaling).astype(jnp.bfloat16))
```

```python
import jax
import jax.numpy as jnp
from jax import lax
from jax.experimental import pallas as pl
from jax.experimental.pallas import tpu as pltpu
from jax.sharding import Mesh
from jax.sharding import PartitionSpec as P

GRADES = 5
LOWEST = -1e30
AXES = ("zh", "x", "y", "zl", "c")
ROWS = ("zh", "x")
COL = ("y", "zl", "c")
SCALE = 1.0 / 32.0
EXP2_SCALE = 1.4426950408889634 / 32.0
BF = jnp.bfloat16
F32 = jnp.float32
LANES = 128


class Wires:
    def __init__(self, send_sems, recv_sems):
        self.send_sems, self.recv_sems = send_sems, recv_sems
        self.names, self.sent = {}, []

    def slot(self, name):
        return self.names.setdefault(name, len(self.names))

    def send(self, src, dst, name, where):
        copy = pltpu.make_async_remote_copy(
            src_ref=src,
            dst_ref=dst,
            send_sem=self.send_sems.at[len(self.sent)],
            recv_sem=self.recv_sems.at[self.slot(name)],
            device_id=where,
            device_id_type=pl.DeviceIdType.MESH,
        )
        copy.start()
        self.sent.append(copy)

    def arrive(self, dst, name, where):
        pltpu.make_async_remote_copy(
            src_ref=dst,
            dst_ref=dst,
            send_sem=self.send_sems.at[0],
            recv_sem=self.recv_sems.at[self.slot(name)],
            device_id=where,
            device_id_type=pl.DeviceIdType.MESH,
        ).wait_recv()

    def finish(self):
        for copy in self.sent:
            copy.wait_send()


def combine(parts):
    row = lax.broadcasted_iota(jnp.int32, (8, LANES), 0)
    stat = row < GRADES
    top = parts[0][0]
    for first, _ in parts[1:]:
        top = jnp.maximum(top, first)
    plain = jnp.zeros((8, LANES), F32)
    mass = jnp.zeros((8, LANES), F32)
    for first, second in parts:
        plain = plain + first
        mass = mass + second * jnp.where(stat, jnp.exp(first - top), 1.0)
    return jnp.where(stat, top, plain), mass


def stacked(rows):
    row = lax.broadcasted_iota(jnp.int32, (8, LANES), 0)
    out = jnp.zeros((8, LANES), F32)
    for k, value in enumerate(rows):
        out = jnp.where(row == k, value, out)
    return out


def outcome(first, second, columns):
    maxima = [first[k : k + 1] for k in range(GRADES)]
    masses = [second[k : k + 1] for k in range(GRADES)]
    counts = [first[5:6], first[6:7], first[7:8], second[5:6], second[6:7]]
    totals = second[7:8]
    levels, running, seen = [], maxima[0], jnp.zeros_like(totals)
    for k in range(GRADES):
        running = jnp.maximum(running, maxima[k])
        seen = seen + counts[k]
        summed = masses[0] * jnp.exp(maxima[0] - running)
        for h in range(1, k + 1):
            summed = summed + masses[h] * jnp.exp(maxima[h] - running)
        present = seen > 0.0
        levels.append(jnp.where(present, running + jnp.log(jnp.where(present, summed, 1.0)), running))
    weighted = counts[0] * levels[0]
    for k in range(1, GRADES):
        weighted = weighted + counts[k] * levels[k]
    losses = (weighted - totals) / columns
    factors = []
    for h in range(GRADES):
        summed = counts[h] * jnp.exp(maxima[h] - levels[h])
        for k in range(h + 1, GRADES):
            summed = summed + counts[k] * jnp.exp(maxima[h] - levels[k])
        factors.append(summed)
    return stacked(maxima), stacked(factors + [losses])


def spread(table, grade):
    return jnp.take_along_axis(table, grade, axis=0, mode="promise_in_bounds")


def kernel(
    q_ref, c_ref, w_ref, g_hbm, loss_ref, qg_ref, cg_ref,
    q_all, c_all, c_par, g_in, g_t, es, sl, sl_par, z_rel, tab, cnt, st, st_in, st_core, res,
    q_part, q_s1, q_r1, q_s2, q_r2, q_s3, q_r3,
    c_part, c_s1, c_r1, c_s2, c_r2, c_s3, c_rel, c_r3,
    send_sems, recv_sems, g_sems,
):
    zh, x, y, zl, c = (lax.axis_index(a) for a in AXES)
    other = 1 - c
    wires = Wires(send_sems, recv_sems)
    send, arrive = wires.send, wires.arrive
    up_y, dn_y = {"y": (y + 1) % 4}, {"y": (y + 3) % 4}
    up_x, dn_x = {"x": (x + 1) % 4}, {"x": (x + 3) % 4}
    mate = {"c": other}
    zl2 = (zl + 2) % 4
    up_zh, dn_zh = (zh + zl // 2) % 2, (zh + 1 + zl // 2) % 2
    up_z, dn_z = {"zh": up_zh, "zl": zl2}, {"zh": dn_zh, "zl": zl2}

    def peer(dy, dz):
        return {"y": (y + dy) % 4, "zl": (zl + dz) % 4}

    others = [(dy, dz) for dy in range(4) for dz in range(4) if (dy, dz) != (0, 0)]

    def q_rows(core, k, dy, start=0, size=64):
        at = core * 1024 + (zl + k) % 4 * 256 + (y + dy) % 4 * 64 + start
        return q_all.at[pl.ds(pl.multiple_of(at, 32), size), :]

    def c_rows(half, dx, start=0, size=128):
        at = half * 512 + (x + dx) % 4 * 128 + start
        return c_all.at[pl.ds(pl.multiple_of(at, 64), size), :]

    def grade_copies(tile):
        core, plane, pair = tile // 8, tile // 2 % 4, tile % 2
        copies = []
        for i in range(2):
            at = (((pair * 2 + i) * 4 + plane) * 2 + core) * 64
            copies.append(
                pltpu.make_async_copy(
                    g_hbm.at[pl.ds(at, 64), :],
                    g_in.at[tile % 4, pl.ds(64 * i, 64), :],
                    g_sems.at[tile % 4, i],
                )
            )
        return copies

    for tile in range(4):
        for copy in grade_copies(tile):
            copy.start()

    barrier = pltpu.get_barrier_semaphore()
    greeted = [peer(dy, dz) for dy, dz in others] + [up_x, dn_x, mate, {"zh": 1 - zh, "zl": zl2}]
    for device in greeted:
        pl.semaphore_signal(barrier, inc=1, device_id=device, device_id_type=pl.DeviceIdType.MESH)
    pl.semaphore_wait(barrier, len(greeted))

    send(q_ref, q_rows(c, 0, 0), ("qy", 0, 0), up_y)
    send(q_ref, q_rows(c, 0, 0), ("qy", 0, 1), dn_y)
    send(c_ref, c_rows(zh, 0), ("cx", 0), up_x)
    send(c_ref, c_rows(zh, 0), ("cx", 1), dn_x)
    send(c_ref.at[pl.ds(0, 64), :], z_rel.at[0], ("zr", 0), up_z)
    send(c_ref.at[pl.ds(64, 64), :], z_rel.at[1], ("zr", 1), dn_z)
    for m in (1, 3, 2):
        send(q_ref, q_rows(c, 0, 0), ("qz", 4 - m), peer(0, m))
    send(q_ref, q_rows(c, 0, 0), ("qd", 0, 0), mate)
    q_rows(c, 0, 0)[...] = q_ref[...]
    c_rows(zh, 0)[...] = c_ref[...]

    def to_mate(k, dy):
        send(q_rows(c, k, dy), q_rows(c, k, dy), ("qd", k, dy), mate)

    def q_near(k):
        arrive(q_rows(c, k, 3), ("qy", k, 0), dn_y)
        send(q_rows(c, k, 3, 0, 32), q_rows(c, k, 3, 0, 32), ("qf", k, 0), up_y)
        to_mate(k, 3)
        arrive(q_rows(c, k, 1), ("qy", k, 1), up_y)
        send(q_rows(c, k, 1, 32, 32), q_rows(c, k, 1, 32, 32), ("qf", k, 1), dn_y)
        to_mate(k, 1)

    def q_far(k):
        arrive(q_rows(c, k, 2, 0, 32), ("qf", k, 0), dn_y)
        arrive(q_rows(c, k, 2, 32, 32), ("qf", k, 1), up_y)
        to_mate(k, 2)

    def q_over(k):
        arrive(q_rows(c, k, 0), ("qz", k), peer(0, k))
        send(q_rows(c, k, 0), q_rows(c, k, 0), ("qy", k, 0), up_y)
        send(q_rows(c, k, 0), q_rows(c, k, 0), ("qy", k, 1), dn_y)
        to_mate(k, 0)

    def c_near():
        arrive(c_rows(zh, 3), ("cx", 0), dn_x)
        send(c_rows(zh, 3, 0, 64), c_rows(zh, 3, 0, 64), ("cf", 0), up_x)
        arrive(c_rows(zh, 1), ("cx", 1), up_x)
        send(c_rows(zh, 1, 64, 64), c_rows(zh, 1, 64, 64), ("cf", 1), dn_x)

    def c_far():
        arrive(c_rows(zh, 2, 0, 64), ("cf", 0), dn_x)
        arrive(c_rows(zh, 2, 64, 64), ("cf", 1), up_x)

    def c_relay():
        arrive(z_rel.at[0], ("zr", 0), dn_z)
        send(z_rel.at[0], c_rows(1 - up_zh, 0, 0, 64), ("cz", 0), up_z)
        arrive(z_rel.at[1], ("zr", 1), up_z)
        send(z_rel.at[1], c_rows(1 - dn_zh, 0, 64, 64), ("cz", 1), dn_z)

    def c_over():
        for h, frm in ((0, dn_z), (1, up_z)):
            part = c_rows(1 - zh, 0, 64 * h, 64)
            arrive(part, ("cz", h), frm)
            send(part, part, ("px", h, 0), up_x)
            send(part, part, ("px", h, 1), dn_x)

    def p_near():
        for h in range(2):
            arrive(c_rows(1 - zh, 3, 64 * h, 64), ("px", h, 0), dn_x)
            if h == 0:
                part = c_rows(1 - zh, 3, 0, 64)
                send(part, part, ("pf", 0), up_x)
            arrive(c_rows(1 - zh, 1, 64 * h, 64), ("px", h, 1), up_x)
            if h == 1:
                part = c_rows(1 - zh, 1, 64, 64)
                send(part, part, ("pf", 1), dn_x)

    def p_far():
        arrive(c_rows(1 - zh, 2, 0, 64), ("pf", 0), dn_x)
        arrive(c_rows(1 - zh, 2, 64, 64), ("pf", 1), up_x)

    def turn(tile):
        for copy in grade_copies(tile):
            copy.wait()
        for b in range(8):
            block = g_in[tile % 4, :, pl.ds(128 * b, 128)]
            g_t[pl.ds(128 * b, 128), pl.ds(128 * tile, 128)] = jnp.transpose(block)
        if tile + 4 < 16:
            for copy in grade_copies(tile + 4):
                copy.start()

        def tally(i, held):
            held = list(held)
            for j in range(8):
                at = pl.multiple_of(i * 64 + 8 * j, 8)
                grade = g_t[pl.ds(at, 8), pl.ds(128 * tile, 128)]
                for k in range(4):
                    held[k] = held[k] + jnp.where(grade == k, 1.0, 0.0)
            return tuple(held)

        held = lax.fori_loop(0, 16, tally, (jnp.zeros((8, LANES), F32),) * 4)
        held = [jnp.sum(v, axis=0, keepdims=True) for v in held]
        held.append(1024.0 - (held[0] + held[1] + held[2] + held[3]))
        cnt[tile] = stacked(held)

    steps = [
        lambda: q_near(0), c_near, c_relay, lambda: q_over(1), lambda: q_over(3), lambda: q_far(0), c_far,
        lambda: q_over(2), lambda: q_near(1), lambda: q_near(3), c_over, lambda: q_near(2), p_near,
        lambda: q_far(1), lambda: q_far(3), lambda: q_far(2), p_far,
    ]
    for n, step in enumerate(steps):
        if n < 16:
            turn(n)
        step()
    send(c_all, c_par, ("cp",), mate)
    for k in range(4):
        for dy in range(4):
            arrive(q_rows(other, k, dy), ("qd", k, dy), mate)

    tab[...] = jnp.zeros_like(tab)

    def tile_stats(tile):
        lanes = pl.ds(pl.multiple_of(tile * LANES, LANES), LANES)

        def highest(i, held):
            held = list(held)
            for j in range(8):
                at = pl.ds(pl.multiple_of(i * 64 + 8 * j, 8), 8)
                score, grade = es[at, lanes], g_t[at, lanes]
                for k in range(GRADES):
                    held[k] = jnp.maximum(held[k], jnp.where(grade == k, score, 32.0 * LOWEST))
                held[GRADES] = held[GRADES] + score
            return tuple(held)

        low = jnp.full((8, LANES), 32.0 * LOWEST, F32)
        held = lax.fori_loop(0, 16, highest, (low,) * GRADES + (jnp.zeros((8, LANES), F32),))
        maxima = [jnp.max(v, axis=0, keepdims=True) for v in held[:GRADES]]
        total = jnp.sum(held[GRADES], axis=0, keepdims=True) * SCALE
        table = stacked(maxima)

        def masses_of(i, held):
            held = list(held)
            for j in range(8):
                at = pl.ds(pl.multiple_of(i * 64 + 8 * j, 8), 8)
                score, grade = es[at, lanes], g_t[at, lanes]
                value = jnp.exp2((score - spread(table, grade)) * EXP2_SCALE)
                es[at, lanes] = value
                for k in range(GRADES):
                    held[k] = held[k] + jnp.where(grade == k, value, 0.0)
            return tuple(held)

        held = lax.fori_loop(0, 16, masses_of, (jnp.zeros((8, LANES), F32),) * GRADES)
        masses = [jnp.sum(v, axis=0, keepdims=True) for v in held]
        counts = [cnt[tile, pl.ds(k, 1), :] for k in range(GRADES)]
        st[tile, pl.ds(0, 8), :] = stacked([m * SCALE for m in maxima] + counts[:3])
        st[tile, pl.ds(8, 8), :] = stacked(masses + counts[3:] + [total])

    def score_tile(n, _):
        rows = pl.ds(pl.multiple_of(n * 256, 256), 256)
        es[:, rows] = lax.dot_general(
            c_all[...], q_all[rows, :], (((1,), (1,)), ((), ())), preferred_element_type=F32
        )
        tile_stats(2 * n)
        tile_stats(2 * n + 1)
        return 0

    lax.fori_loop(0, 8, score_tile, 0)

    mine = y * 4 + zl
    for dy, dz in others:
        target = (y + dy) % 4 * 4 + (zl + dz) % 4
        send(st.at[target], st_in.at[dy * 4 + dz], ("st", dy, dz), peer(dy, dz))
    parts = [(st[mine, pl.ds(0, 8), :], st[mine, pl.ds(8, 8), :])]
    for dy, dz in others:
        arrive(st_in.at[dy * 4 + dz], ("st", dy, dz), peer(4 - dy, 4 - dz))
        parts.append((st_in[dy * 4 + dz, pl.ds(0, 8), :], st_in[dy * 4 + dz, pl.ds(8, 8), :]))
    first, second = combine(parts)
    st_core[0, pl.ds(0, 8), :] = first
    st_core[0, pl.ds(8, 8), :] = second
    send(st_core.at[0], st_core.at[1], ("sd",), mate)
    arrive(st_core.at[1], ("sd",), mate)
    first, second = combine([(first, second), (st_core[1, pl.ds(0, 8), :], st_core[1, pl.ds(8, 8), :])])
    first, second = outcome(first, second, 32768.0)
    res[mine, pl.ds(0, 8), :] = first
    res[mine, pl.ds(8, 8), :] = second
    for dy, dz in others:
        send(res.at[mine], res.at[mine], ("sr", dy, dz), peer(dy, dz))
    arrive(c_par, ("cp",), mate)
    for dy, dz in others:
        source = (y + 4 - dy) % 4 * 4 + (zl + 4 - dz) % 4
        arrive(res.at[source], ("sr", dy, dz), peer(4 - dy, 4 - dz))
    loss_ref[...] = res[:, 13, :]

    def slope_tile(tile):
        lanes = pl.ds(pl.multiple_of(tile * LANES, LANES), LANES)
        weight = w_ref[pl.ds(tile, 1), :] * SCALE
        table = res[tile, pl.ds(8, 8), :] * jnp.exp(st[tile, pl.ds(0, 8), :] - res[tile, pl.ds(0, 8), :])
        row = lax.broadcasted_iota(jnp.int32, (8, LANES), 0)
        table = jnp.where(row < GRADES, table, 0.0) * weight

        def at_rows(i, _):
            for j in range(4):
                at = pl.multiple_of(i * 64 + 16 * j, 16)
                halves = []
                for h in range(2):
                    rows = pl.ds(pl.multiple_of(at + 8 * h, 8), 8)
                    halves.append(spread(table, g_t[rows, lanes]) * es[rows, lanes] - weight)
                sl[pl.ds(at, 16), lanes] = jnp.concatenate(halves, axis=0).astype(BF)
            return 0

        lax.fori_loop(0, 16, at_rows, 0)

    def lanes_of(core, plane):
        return pl.ds(pl.multiple_of(core * 1024 + plane * 256, 256), 256)

    for k in (1, 2, 3, 0):
        plane = (zl + k) % 4
        slope_tile(other * 8 + plane * 2)
        slope_tile(other * 8 + plane * 2 + 1)
        lanes = lanes_of(other, plane)
        send(sl.at[:, lanes], sl_par.at[:, lanes_of(0, plane)], ("sl", k), mate)
    for k in (1, 2, 3, 0):
        plane = (zl + k) % 4
        slope_tile(c * 8 + plane * 2)
        slope_tile(c * 8 + plane * 2 + 1)

    def c_dot(j):
        half = (zh + 1 - j) % 2
        for i in range(2):
            rows = pl.ds(pl.multiple_of(half * 512 + 256 * i, 256), 256)
            c_part[j, pl.ds(256 * i, 256), :] = jnp.dot(sl[rows, :], q_all[...], preferred_element_type=F32)

        def at(d, start, size):
            return pl.ds(pl.multiple_of((x + d) % 4 * 128 + start, 64), size)

        c_s1[j, 0] = c_part[j, at(2, 0, 64), :].astype(BF)
        c_s1[j, 1] = c_part[j, at(2, 64, 64), :].astype(BF)
        send(c_s1.at[j, 0], c_r1.at[j, 0], ("s1", j, 0), up_x)
        send(c_s1.at[j, 1], c_r1.at[j, 1], ("s1", j, 1), dn_x)

    def c_mid(j):
        def at(d, start, size):
            return pl.ds(pl.multiple_of((x + d) % 4 * 128 + start, 64), size)

        arrive(c_r1.at[j, 0], ("s1", j, 0), dn_x)
        c_s2[j, 0, pl.ds(0, 64), :] = (c_part[j, at(1, 0, 64), :] + c_r1[j, 0].astype(F32)).astype(BF)
        c_s2[j, 0, pl.ds(64, 64), :] = c_part[j, at(1, 64, 64), :].astype(BF)
        send(c_s2.at[j, 0], c_r2.at[j, 0], ("s2", j, 0), up_x)
        arrive(c_r1.at[j, 1], ("s1", j, 1), up_x)
        c_s2[j, 1, pl.ds(0, 64), :] = c_part[j, at(3, 0, 64), :].astype(BF)
        c_s2[j, 1, pl.ds(64, 64), :] = (c_part[j, at(3, 64, 64), :] + c_r1[j, 1].astype(F32)).astype(BF)
        send(c_s2.at[j, 1], c_r2.at[j, 1], ("s2", j, 1), dn_x)

    def c_sum(j):
        arrive(c_r2.at[j, 0], ("s2", j, 0), dn_x)
        arrive(c_r2.at[j, 1], ("s2", j, 1), up_x)
        at = pl.ds(pl.multiple_of(x * 128, 128), 128)
        return c_part[j, at, :] + c_r2[j, 0].astype(F32) + c_r2[j, 1].astype(F32)

    def c_leave():
        c_s3[...] = c_sum(0).astype(BF)
        send(c_s3.at[pl.ds(0, 64), :], c_rel.at[0], ("t1", 0), up_z)
        send(c_s3.at[pl.ds(64, 64), :], c_rel.at[1], ("t1", 1), dn_z)

    def c_pass():
        arrive(c_rel.at[0], ("t1", 0), dn_z)
        send(c_rel.at[0], c_r3.at[pl.ds(0, 64), :], ("t2", 0), up_z)
        arrive(c_rel.at[1], ("t1", 1), up_z)
        send(c_rel.at[1], c_r3.at[pl.ds(64, 64), :], ("t2", 1), dn_z)

    def c_end():
        total = c_sum(1)
        arrive(c_r3.at[pl.ds(0, 64), :], ("t2", 0), dn_z)
        arrive(c_r3.at[pl.ds(64, 64), :], ("t2", 1), up_z)
        cg_ref[...] = (total + c_r3[...].astype(F32)).astype(BF)

    dims = (((0,), (0,)), ((), ()))

    def q_dot(k):
        plane = (zl + k) % 4
        arrive(sl_par.at[:, lanes_of(0, plane)], ("sl", k), mate)
        q_part[k] = lax.dot_general(
            sl[:, lanes_of(c, plane)], c_all[...], dims, preferred_element_type=F32
        ) + lax.dot_general(sl_par[:, lanes_of(0, plane)], c_par[...], dims, preferred_element_type=F32)

        def at(d, start, size):
            return pl.ds(pl.multiple_of((y + d) % 4 * 64 + start, 32), size)

        q_s1[k, 0] = q_part[k, at(2, 0, 32), :].astype(BF)
        q_s1[k, 1] = q_part[k, at(2, 32, 32), :].astype(BF)
        send(q_s1.at[k, 0], q_r1.at[k, 0], ("r1", k, 0), up_y)
        send(q_s1.at[k, 1], q_r1.at[k, 1], ("r1", k, 1), dn_y)

    def q_mid(k):
        def at(d, start, size):
            return pl.ds(pl.multiple_of((y + d) % 4 * 64 + start, 32), size)

        arrive(q_r1.at[k, 0], ("r1", k, 0), dn_y)
        q_s2[k, 0, pl.ds(0, 32), :] = (q_part[k, at(1, 0, 32), :] + q_r1[k, 0].astype(F32)).astype(BF)
        q_s2[k, 0, pl.ds(32, 32), :] = q_part[k, at(1, 32, 32), :].astype(BF)
        send(q_s2.at[k, 0], q_r2.at[k, 0], ("r2", k, 0), up_y)
        arrive(q_r1.at[k, 1], ("r1", k, 1), up_y)
        q_s2[k, 1, pl.ds(0, 32), :] = q_part[k, at(3, 0, 32), :].astype(BF)
        q_s2[k, 1, pl.ds(32, 32), :] = (q_part[k, at(3, 32, 32), :] + q_r1[k, 1].astype(F32)).astype(BF)
        send(q_s2.at[k, 1], q_r2.at[k, 1], ("r2", k, 1), dn_y)

    def q_sum(k):
        arrive(q_r2.at[k, 0], ("r2", k, 0), dn_y)
        arrive(q_r2.at[k, 1], ("r2", k, 1), up_y)
        at = pl.ds(pl.multiple_of(y * 64, 64), 64)
        return q_part[k, at, :] + q_r2[k, 0].astype(F32) + q_r2[k, 1].astype(F32)

    def q_leave(k):
        q_s3[k - 1] = q_sum(k).astype(BF)
        send(q_s3.at[k - 1], q_r3.at[3 - k], ("r3", 4 - k), peer(0, k))

    def q_end():
        total = q_sum(0)
        for k in (1, 3, 2):
            arrive(q_r3.at[k - 1], ("r3", k), peer(0, k))
            total = total + q_r3[k - 1].astype(F32)
        qg_ref[...] = total.astype(BF)

    c_dot(0)
    q_dot(1)
    q_dot(2)
    c_mid(0)
    q_mid(1)
    c_dot(1)
    q_mid(2)
    q_dot(3)
    q_dot(0)
    c_mid(1)
    q_mid(3)
    q_leave(1)
    c_leave()
    q_mid(0)
    q_leave(2)
    q_leave(3)
    c_pass()
    q_end()
    c_end()
    wires.finish()


def local(queries, candidates, grades, query_weights):
    vmem = pl.BlockSpec(memory_space=pltpu.VMEM)
    weights = query_weights.reshape(4, 4, 2, 64).transpose(2, 1, 0, 3).reshape(16, LANES)
    shapes = [
        ((2048, 1024), BF), ((1024, 1024), BF), ((1024, 1024), BF), ((4, 128, 1024), jnp.int32),
        ((1024, 2048), jnp.int32), ((1024, 2048), F32), ((1024, 2048), BF), ((1024, 1024), BF),
        ((2, 64, 1024), BF), ((8, LANES), F32), ((16, 8, LANES), F32), ((16, 16, LANES), F32),
        ((16, 16, LANES), F32), ((2, 16, LANES), F32), ((16, 16, LANES), F32),
        ((4, 256, 1024), F32), ((4, 2, 32, 1024), BF), ((4, 2, 32, 1024), BF), ((4, 2, 64, 1024), BF),
        ((4, 2, 64, 1024), BF), ((3, 64, 1024), BF), ((3, 64, 1024), BF),
        ((2, 512, 1024), F32), ((2, 2, 64, 1024), BF), ((2, 2, 64, 1024), BF), ((2, 2, 128, 1024), BF),
        ((2, 2, 128, 1024), BF), ((128, 1024), BF), ((2, 64, 1024), BF), ((128, 1024), BF),
    ]
    losses, query_grad, cand_grad = pl.pallas_call(
        kernel,
        out_shape=(
            jax.ShapeDtypeStruct((16, LANES), F32),
            jax.ShapeDtypeStruct((64, 1024), BF),
            jax.ShapeDtypeStruct((128, 1024), BF),
        ),
        in_specs=[vmem, vmem, vmem, pl.BlockSpec(memory_space=pl.ANY)],
        out_specs=(vmem, vmem, vmem),
        scratch_shapes=[pltpu.VMEM(shape, dtype) for shape, dtype in shapes]
        + [
            pltpu.SemaphoreType.DMA((160,)),
            pltpu.SemaphoreType.DMA((160,)),
            pltpu.SemaphoreType.DMA((4, 2)),
        ],
        compiler_params=pltpu.CompilerParams(
            collective_id=0, has_side_effects=True, vmem_limit_bytes=66 * 1000 * 1000
        ),
        name="listmle",
    )(queries, candidates, weights, grades)
    losses = losses.reshape(2, 4, 4, 64).transpose(2, 1, 0, 3).reshape(2048)
    return losses, query_grad, cand_grad


def solution(mesh):
    split = Mesh(mesh.devices.reshape(2, 4, 4, 4, 2), AXES)
    return jax.shard_map(
        local,
        mesh=split,
        in_specs=(P(AXES_Q := ROWS + COL, None), P(COL + ROWS, None), P(ROWS, COL), P(ROWS)),
        out_specs=(P(ROWS), P(AXES_Q, None), P(COL + ROWS, None)),
        check_vma=False,
    )
```

```python
import jax
import jax.numpy as jnp
from jax import lax
from jax.experimental import pallas as pl
from jax.experimental.pallas import tpu as pltpu
from jax.sharding import Mesh
from jax.sharding import PartitionSpec as P

GRADES = 5
LOWEST = -1e30
AXES = ("zh", "x", "y", "zl", "c")
ROWS = ("zh", "x")
COL = ("y", "zl", "c")
SCALE = 1.0 / 32.0
EXP2_SCALE = 1.4426950408889634 / 32.0
BF = jnp.bfloat16
F32 = jnp.float32
LANES = 128


class Wires:
    def __init__(self, send_sems, recv_sems):
        self.send_sems, self.recv_sems = send_sems, recv_sems
        self.names, self.sent = {}, []

    def slot(self, name):
        return self.names.setdefault(name, len(self.names))

    def send(self, src, dst, name, where):
        copy = pltpu.make_async_remote_copy(
            src_ref=src,
            dst_ref=dst,
            send_sem=self.send_sems.at[len(self.sent)],
            recv_sem=self.recv_sems.at[self.slot(name)],
            device_id=where,
            device_id_type=pl.DeviceIdType.MESH,
        )
        copy.start()
        self.sent.append(copy)

    def arrive(self, dst, name, where):
        pltpu.make_async_remote_copy(
            src_ref=dst,
            dst_ref=dst,
            send_sem=self.send_sems.at[0],
            recv_sem=self.recv_sems.at[self.slot(name)],
            device_id=where,
            device_id_type=pl.DeviceIdType.MESH,
        ).wait_recv()

    def finish(self):
        for copy in self.sent:
            copy.wait_send()


def combine(parts):
    row = lax.broadcasted_iota(jnp.int32, (8, LANES), 0)
    stat = row < GRADES
    top = parts[0][0]
    for first, _ in parts[1:]:
        top = jnp.maximum(top, first)
    plain = jnp.zeros((8, LANES), F32)
    mass = jnp.zeros((8, LANES), F32)
    for first, second in parts:
        plain = plain + first
        mass = mass + second * jnp.where(stat, jnp.exp(first - top), 1.0)
    return jnp.where(stat, top, plain), mass


def stacked(rows):
    row = lax.broadcasted_iota(jnp.int32, (8, LANES), 0)
    out = jnp.zeros((8, LANES), F32)
    for k, value in enumerate(rows):
        out = jnp.where(row == k, value, out)
    return out


def outcome(first, second, columns):
    maxima = [first[k : k + 1] for k in range(GRADES)]
    masses = [second[k : k + 1] for k in range(GRADES)]
    counts = [first[5:6], first[6:7], first[7:8], second[5:6], second[6:7]]
    totals = second[7:8]
    levels, running, seen = [], maxima[0], jnp.zeros_like(totals)
    for k in range(GRADES):
        running = jnp.maximum(running, maxima[k])
        seen = seen + counts[k]
        summed = masses[0] * jnp.exp(maxima[0] - running)
        for h in range(1, k + 1):
            summed = summed + masses[h] * jnp.exp(maxima[h] - running)
        present = seen > 0.0
        levels.append(jnp.where(present, running + jnp.log(jnp.where(present, summed, 1.0)), running))
    weighted = counts[0] * levels[0]
    for k in range(1, GRADES):
        weighted = weighted + counts[k] * levels[k]
    losses = (weighted - totals) / columns
    factors = []
    for h in range(GRADES):
        summed = counts[h] * jnp.exp(maxima[h] - levels[h])
        for k in range(h + 1, GRADES):
            summed = summed + counts[k] * jnp.exp(maxima[h] - levels[k])
        factors.append(summed)
    return stacked(maxima), stacked(factors + [losses])


GATHER = lax.GatherDimensionNumbers(
    offset_dims=(),
    collapsed_slice_dims=(0,),
    start_index_map=(0,),
    operand_batching_dims=(1,),
    start_indices_batching_dims=(1,),
)


def spread(table, grade):
    pieces = [
        lax.gather(
            table,
            grade[at : at + 8][..., None],
            GATHER,
            slice_sizes=(1, 1),
            mode=lax.GatherScatterMode.PROMISE_IN_BOUNDS,
        )
        for at in range(0, grade.shape[0], 8)
    ]
    return jnp.concatenate(pieces, axis=0)


def folded(op, block):
    return op(block.reshape(-1, 8, LANES), axis=0)


def kernel(
    q_ref, c_ref, w_ref, g_hbm, loss_ref, qg_ref, cg_ref,
    q_all, c_all, c_par, w_t, g_in, g_t, es, sl, sl_par, z_rel, cnt, st_half, st, st_in, st_core, res,
    q_part, q_s1, q_r1, q_s2, q_r2, q_s3, q_r3,
    c_part, c_s1, c_r1, c_s2, c_r2, c_s3, c_rel, c_r3,
    send_sems, recv_sems, g_sems,
):
    zh, x, y, zl, c = (lax.axis_index(a) for a in AXES)
    other = 1 - c
    wires = Wires(send_sems, recv_sems)
    send, arrive = wires.send, wires.arrive
    up_y, dn_y = {"y": (y + 1) % 4}, {"y": (y + 3) % 4}
    up_x, dn_x = {"x": (x + 1) % 4}, {"x": (x + 3) % 4}
    mate = {"c": other}
    zl2 = (zl + 2) % 4
    planes = (zl, zl + 1 - 2 * (zl % 2), zl2, 3 - zl)
    up_zh, dn_zh = (zh + zl // 2) % 2, (zh + 1 + zl // 2) % 2
    up_z, dn_z = {"zh": up_zh, "zl": zl2}, {"zh": dn_zh, "zl": zl2}

    def peer(dy, dz):
        return {"y": (y + dy) % 4, "zl": (zl + dz) % 4}

    others = [(dy, dz) for dy in range(4) for dz in range(4) if (dy, dz) != (0, 0)]

    def q_rows(core, k, dy, start=0, size=64):
        at = core * 1024 + planes[k] * 256 + (y + dy) % 4 * 64 + start
        return q_all.at[pl.ds(pl.multiple_of(at, 32), size), :]

    def c_rows(half, dx, start=0, size=128):
        at = half * 512 + (x + dx) % 4 * 128 + start
        return c_all.at[pl.ds(pl.multiple_of(at, 64), size), :]

    def grade_copies(tile):
        core, plane, pair = tile // 8, tile // 2 % 4, tile % 2
        copies = []
        for i in range(2):
            at = (((pair * 2 + i) * 4 + plane) * 2 + core) * 64
            copies.append(
                pltpu.make_async_copy(
                    g_hbm.at[pl.ds(at, 64), :],
                    g_in.at[tile % 4, pl.ds(64 * i, 64), :],
                    g_sems.at[tile % 4, i],
                )
            )
        return copies

    for tile in range(4):
        for copy in grade_copies(tile):
            copy.start()

    barrier = pltpu.get_barrier_semaphore()
    greeted = [{"zl": planes[k]} for k in (1, 2, 3)] + [up_y, dn_y, up_x, dn_x, mate, {"zh": 1 - zh, "zl": zl2}]
    for device in greeted:
        pl.semaphore_signal(barrier, inc=1, device_id=device, device_id_type=pl.DeviceIdType.MESH)
    pl.semaphore_wait(barrier, len(greeted))

    send(q_ref, q_rows(c, 0, 0), ("qy", 0, 0), up_y)
    send(q_ref, q_rows(c, 0, 0), ("qy", 0, 1), dn_y)
    send(c_ref, c_rows(zh, 0), ("cx", 0), up_x)
    send(c_ref, c_rows(zh, 0), ("cx", 1), dn_x)
    send(c_ref.at[pl.ds(0, 64), :], z_rel.at[0], ("zr", 0), up_z)
    send(c_ref.at[pl.ds(64, 64), :], z_rel.at[1], ("zr", 1), dn_z)
    for k in (1, 2, 3):
        send(q_ref, q_rows(c, 0, 0), ("qz", k), {"zl": planes[k]})
    send(q_ref, q_rows(c, 0, 0), ("qd", 0, 0), mate)
    for t in range(16):
        core, at = t // 8, t % 2 * 8 + t // 2 % 4
        pair = [w_ref[pl.ds(at, 1), :], w_ref[pl.ds(at + 4, 1), :]]
        pair[1 - core] = pltpu.roll(pair[1 - core], 64, 1)
        w_t[pl.ds(t, 1), :] = jnp.where(lax.broadcasted_iota(jnp.int32, (1, LANES), 1) < 64, *pair)
    q_rows(c, 0, 0)[...] = q_ref[...]
    c_rows(zh, 0)[...] = c_ref[...]

    def to_mate(k, dy):
        send(q_rows(c, k, dy), q_rows(c, k, dy), ("qd", k, dy), mate)

    def q_near(k):
        arrive(q_rows(c, k, 3), ("qy", k, 0), dn_y)
        send(q_rows(c, k, 3, 0, 32), q_rows(c, k, 3, 0, 32), ("qf", k, 0), up_y)
        to_mate(k, 3)
        arrive(q_rows(c, k, 1), ("qy", k, 1), up_y)
        send(q_rows(c, k, 1, 32, 32), q_rows(c, k, 1, 32, 32), ("qf", k, 1), dn_y)
        to_mate(k, 1)

    def q_far(k):
        arrive(q_rows(c, k, 2, 0, 32), ("qf", k, 0), dn_y)
        arrive(q_rows(c, k, 2, 32, 32), ("qf", k, 1), up_y)
        to_mate(k, 2)

    def q_over(k):
        arrive(q_rows(c, k, 0), ("qz", k), {"zl": planes[k]})
        send(q_rows(c, k, 0), q_rows(c, k, 0), ("qy", k, 0), up_y)
        send(q_rows(c, k, 0), q_rows(c, k, 0), ("qy", k, 1), dn_y)
        to_mate(k, 0)

    def c_near():
        arrive(c_rows(zh, 3), ("cx", 0), dn_x)
        send(c_rows(zh, 3, 0, 64), c_rows(zh, 3, 0, 64), ("cf", 0), up_x)
        arrive(c_rows(zh, 1), ("cx", 1), up_x)
        send(c_rows(zh, 1, 64, 64), c_rows(zh, 1, 64, 64), ("cf", 1), dn_x)

    def c_far():
        arrive(c_rows(zh, 2, 0, 64), ("cf", 0), dn_x)
        arrive(c_rows(zh, 2, 64, 64), ("cf", 1), up_x)

    def c_relay():
        arrive(z_rel.at[0], ("zr", 0), dn_z)
        send(z_rel.at[0], c_rows(1 - up_zh, 0, 0, 64), ("cz", 0), up_z)
        arrive(z_rel.at[1], ("zr", 1), up_z)
        send(z_rel.at[1], c_rows(1 - dn_zh, 0, 64, 64), ("cz", 1), dn_z)

    def c_over():
        for h, frm in ((0, dn_z), (1, up_z)):
            part = c_rows(1 - zh, 0, 64 * h, 64)
            arrive(part, ("cz", h), frm)
            send(part, part, ("px", h, 0), up_x)
            send(part, part, ("px", h, 1), dn_x)

    def p_near():
        for h in range(2):
            arrive(c_rows(1 - zh, 3, 64 * h, 64), ("px", h, 0), dn_x)
            if h == 0:
                part = c_rows(1 - zh, 3, 0, 64)
                send(part, part, ("pf", 0), up_x)
            arrive(c_rows(1 - zh, 1, 64 * h, 64), ("px", h, 1), up_x)
            if h == 1:
                part = c_rows(1 - zh, 1, 64, 64)
                send(part, part, ("pf", 1), dn_x)

    def p_far():
        arrive(c_rows(1 - zh, 2, 0, 64), ("pf", 0), dn_x)
        arrive(c_rows(1 - zh, 2, 64, 64), ("pf", 1), up_x)

    def turn(tile):
        for copy in grade_copies(tile):
            copy.wait()
        for b in range(8):
            block = g_in[tile % 4, :, pl.ds(128 * b, 128)]
            g_t[pl.ds(128 * b, 128), pl.ds(128 * tile, 128)] = jnp.transpose(block)
        if tile + 4 < 16:
            for copy in grade_copies(tile + 4):
                copy.start()

        for h in range(2):

            def tally(i, held):
                at = pl.ds(pl.multiple_of(h * 512 + i * 64, 64), 64)
                grade = g_t[at, pl.ds(128 * tile, 128)]
                return tuple(v + folded(jnp.sum, jnp.where(grade == k, 1.0, 0.0)) for k, v in enumerate(held))

            held = lax.fori_loop(0, 8, tally, (jnp.zeros((8, LANES), F32),) * 4)
            held = [jnp.sum(v, axis=0, keepdims=True) for v in held]
            held.append(512.0 - (held[0] + held[1] + held[2] + held[3]))
            cnt[h, tile] = stacked(held)

    def tile_stats(half, tile):
        lanes = pl.ds(pl.multiple_of(tile * LANES, LANES), LANES)

        def highest(i, held):
            at = pl.ds(pl.multiple_of(half * 512 + i * 64, 64), 64)
            score, grade = es[at, lanes], g_t[at, lanes]
            new = [
                jnp.maximum(held[k], folded(jnp.max, jnp.where(grade == k, score, 32.0 * LOWEST)))
                for k in range(GRADES)
            ]
            return (*new, held[GRADES] + folded(jnp.sum, score))

        low = jnp.full((8, LANES), 32.0 * LOWEST, F32)
        held = lax.fori_loop(0, 8, highest, (low,) * GRADES + (jnp.zeros((8, LANES), F32),))
        maxima = [jnp.max(v, axis=0, keepdims=True) for v in held[:GRADES]]
        total = jnp.sum(held[GRADES], axis=0, keepdims=True) * SCALE
        table = stacked(maxima)

        def masses_of(i, held):
            at = pl.ds(pl.multiple_of(half * 512 + i * 64, 64), 64)
            score, grade = es[at, lanes], g_t[at, lanes]
            value = jnp.exp2((score - spread(table, grade)) * EXP2_SCALE)
            es[at, lanes] = value
            return tuple(
                held[k] + folded(jnp.sum, jnp.where(grade == k, value, 0.0)) for k in range(GRADES)
            )

        held = lax.fori_loop(0, 8, masses_of, (jnp.zeros((8, LANES), F32),) * GRADES)
        masses = [jnp.sum(v, axis=0, keepdims=True) for v in held]
        counts = [cnt[half, tile, pl.ds(k, 1), :] for k in range(GRADES)]
        st_half[half, tile, pl.ds(0, 8), :] = stacked([m * SCALE for m in maxima] + counts[:3])
        st_half[half, tile, pl.ds(8, 8), :] = stacked(masses + counts[3:] + [total])

    def unit(h, k):
        half = (zh + h) % 2
        cands = pl.ds(pl.multiple_of(half * 512, 512), 512)

        def one(core, _):
            n = core * 4 + planes[k]
            rows = pl.ds(pl.multiple_of(n * 256, 256), 256)
            es[cands, rows] = lax.dot_general(
                c_all[cands, :], q_all[rows, :], (((1,), (1,)), ((), ())), preferred_element_type=F32
            )
            tile_stats(half, 2 * n)
            tile_stats(half, 2 * n + 1)
            return 0

        lax.fori_loop(0, 2, one, 0)

    def turns(first, last):
        for tile in range(first, last):
            turn(tile)

    def q_mate(k):
        for dy in range(4):
            arrive(q_rows(other, k, dy), ("qd", k, dy), mate)

    steps = [
        (turns, 0, 8), (q_near, 0), (turns, 8, 12), (c_near,), (c_relay,), (turns, 12, 16), (q_over, 1), (q_far, 0),
        (c_far,), (q_mate, 0), (unit, 0, 0), (q_over, 2), (q_near, 1), (c_over,), (q_over, 3), (q_far, 1), (q_near, 2),
        (p_near,), (q_near, 3), (q_mate, 1), (unit, 0, 1), (q_far, 2), (p_far,),
        (send, c_all, c_par, ("cp",), mate), (q_mate, 2), (unit, 0, 2), (unit, 1, 0), (q_far, 3), (unit, 1, 1),
        (q_mate, 3), (unit, 0, 3), (unit, 1, 2), (unit, 1, 3),
    ]
    for step, *given in steps:
        step(*given)

    for t in range(16):
        first, second = combine(
            [(st_half[h, t, pl.ds(0, 8), :], st_half[h, t, pl.ds(8, 8), :]) for h in range(2)]
        )
        st[t, pl.ds(0, 8), :] = first
        st[t, pl.ds(8, 8), :] = second

    mine = y * 4 + zl
    for dy, dz in others:
        target = (y + dy) % 4 * 4 + (zl + dz) % 4
        send(st.at[target], st_in.at[dy * 4 + dz], ("st", dy, dz), peer(dy, dz))
    parts = [(st[mine, pl.ds(0, 8), :], st[mine, pl.ds(8, 8), :])]
    for dy, dz in others:
        arrive(st_in.at[dy * 4 + dz], ("st", dy, dz), peer(4 - dy, 4 - dz))
        parts.append((st_in[dy * 4 + dz, pl.ds(0, 8), :], st_in[dy * 4 + dz, pl.ds(8, 8), :]))
    first, second = combine(parts)
    st_core[0, pl.ds(0, 8), :] = first
    st_core[0, pl.ds(8, 8), :] = second
    send(st_core.at[0], st_core.at[1], ("sd",), mate)
    arrive(st_core.at[1], ("sd",), mate)
    first, second = combine([(first, second), (st_core[1, pl.ds(0, 8), :], st_core[1, pl.ds(8, 8), :])])
    first, second = outcome(first, second, 32768.0)
    res[mine, pl.ds(0, 8), :] = first
    res[mine, pl.ds(8, 8), :] = second
    for dy, dz in others:
        send(res.at[mine], res.at[mine], ("sr", dy, dz), peer(dy, dz))
    arrive(c_par, ("cp",), mate)
    for dy, dz in others:
        source = (y + 4 - dy) % 4 * 4 + (zl + 4 - dz) % 4
        arrive(res.at[source], ("sr", dy, dz), peer(4 - dy, 4 - dz))
    found = [res[t, pl.ds(13, 1), :] for t in range(16)]
    low_lanes = lax.broadcasted_iota(jnp.int32, (1, LANES), 1) < 64
    for v in range(4):
        for p in range(4):
            pair = [found[core * 8 + p * 2 + v // 2] for core in range(2)]
            pair[1 - v % 2] = pltpu.roll(pair[1 - v % 2], 64, 1)
            loss_ref[pl.ds(v * 4 + p, 1), :] = jnp.where(low_lanes, pair[0], pair[1])

    def slope_tile(half, tile):
        lanes = pl.ds(pl.multiple_of(tile * LANES, LANES), LANES)
        weight = w_t[pl.ds(tile, 1), :] * SCALE
        table = res[tile, pl.ds(8, 8), :] * jnp.exp(st_half[half, tile, pl.ds(0, 8), :] - res[tile, pl.ds(0, 8), :])
        row = lax.broadcasted_iota(jnp.int32, (8, LANES), 0)
        table = jnp.where(row < GRADES, table, 0.0) * weight

        def at_rows(i, _):
            at = pl.ds(pl.multiple_of(half * 512 + i * 64, 64), 64)
            sl[at, lanes] = (spread(table, g_t[at, lanes]) * es[at, lanes] - weight).astype(BF)
            return 0

        lax.fori_loop(0, 8, at_rows, 0)

    def lanes_of(core, plane):
        return pl.ds(pl.multiple_of(core * 1024 + plane * 256, 256), 256)

    def slopes(j):
        half = (zh + 1 - j) % 2
        cands = pl.ds(pl.multiple_of(half * 512, 512), 512)

        def one(t, core):
            slope_tile(half, core * 8 + t)
            return core

        lax.fori_loop(0, 8, one, other)
        send(sl.at[cands, pl.ds(pl.multiple_of(other * 1024, 1024), 1024)], sl_par.at[cands, :], ("sl", j), mate)
        lax.fori_loop(0, 8, one, c)

    def slopes_mate(j):
        cands = pl.ds(pl.multiple_of((zh + 1 - j) % 2 * 512, 512), 512)
        arrive(sl_par.at[cands, :], ("sl", j), mate)

    def c_dot(j):
        half = (zh + 1 - j) % 2
        for i in range(2):
            rows = pl.ds(pl.multiple_of(half * 512 + 256 * i, 256), 256)
            c_part[j, pl.ds(256 * i, 256), :] = jnp.dot(sl[rows, :], q_all[...], preferred_element_type=F32)

        def at(d, start, size):
            return pl.ds(pl.multiple_of((x + d) % 4 * 128 + start, 64), size)

        c_s1[j, 0] = c_part[j, at(2, 0, 64), :].astype(BF)
        c_s1[j, 1] = c_part[j, at(2, 64, 64), :].astype(BF)
        send(c_s1.at[j, 0], c_r1.at[j, 0], ("s1", j, 0), up_x)
        send(c_s1.at[j, 1], c_r1.at[j, 1], ("s1", j, 1), dn_x)

    def c_mid(j):
        def at(d, start, size):
            return pl.ds(pl.multiple_of((x + d) % 4 * 128 + start, 64), size)

        arrive(c_r1.at[j, 0], ("s1", j, 0), dn_x)
        c_s2[j, 0, pl.ds(0, 64), :] = (c_part[j, at(1, 0, 64), :] + c_r1[j, 0].astype(F32)).astype(BF)
        c_s2[j, 0, pl.ds(64, 64), :] = c_part[j, at(1, 64, 64), :].astype(BF)
        send(c_s2.at[j, 0], c_r2.at[j, 0], ("s2", j, 0), up_x)
        arrive(c_r1.at[j, 1], ("s1", j, 1), up_x)
        c_s2[j, 1, pl.ds(0, 64), :] = c_part[j, at(3, 0, 64), :].astype(BF)
        c_s2[j, 1, pl.ds(64, 64), :] = (c_part[j, at(3, 64, 64), :] + c_r1[j, 1].astype(F32)).astype(BF)
        send(c_s2.at[j, 1], c_r2.at[j, 1], ("s2", j, 1), dn_x)

    def c_sum(j):
        arrive(c_r2.at[j, 0], ("s2", j, 0), dn_x)
        arrive(c_r2.at[j, 1], ("s2", j, 1), up_x)
        at = pl.ds(pl.multiple_of(x * 128, 128), 128)
        return c_part[j, at, :] + c_r2[j, 0].astype(F32) + c_r2[j, 1].astype(F32)

    def c_leave():
        c_s3[...] = c_sum(0).astype(BF)
        send(c_s3.at[pl.ds(0, 64), :], c_rel.at[0], ("t1", 0), up_z)
        send(c_s3.at[pl.ds(64, 64), :], c_rel.at[1], ("t1", 1), dn_z)

    def c_pass():
        arrive(c_rel.at[0], ("t1", 0), dn_z)
        send(c_rel.at[0], c_r3.at[pl.ds(0, 64), :], ("t2", 0), up_z)
        arrive(c_rel.at[1], ("t1", 1), up_z)
        send(c_rel.at[1], c_r3.at[pl.ds(64, 64), :], ("t2", 1), dn_z)

    def c_end():
        total = c_sum(1)
        arrive(c_r3.at[pl.ds(0, 64), :], ("t2", 0), dn_z)
        arrive(c_r3.at[pl.ds(64, 64), :], ("t2", 1), up_z)
        cg_ref[...] = (total + c_r3[...].astype(F32)).astype(BF)

    dims = (((0,), (0,)), ((), ()))

    def q_dot(k):
        plane = planes[k]
        q_part[k] = lax.dot_general(
            sl[:, lanes_of(c, plane)], c_all[...], dims, preferred_element_type=F32
        ) + lax.dot_general(sl_par[:, lanes_of(0, plane)], c_par[...], dims, preferred_element_type=F32)

        def at(d, start, size):
            return pl.ds(pl.multiple_of((y + d) % 4 * 64 + start, 32), size)

        q_s1[k, 0] = q_part[k, at(2, 0, 32), :].astype(BF)
        q_s1[k, 1] = q_part[k, at(2, 32, 32), :].astype(BF)
        send(q_s1.at[k, 0], q_r1.at[k, 0], ("r1", k, 0), up_y)
        send(q_s1.at[k, 1], q_r1.at[k, 1], ("r1", k, 1), dn_y)

    def q_mid(k):
        def at(d, start, size):
            return pl.ds(pl.multiple_of((y + d) % 4 * 64 + start, 32), size)

        arrive(q_r1.at[k, 0], ("r1", k, 0), dn_y)
        q_s2[k, 0, pl.ds(0, 32), :] = (q_part[k, at(1, 0, 32), :] + q_r1[k, 0].astype(F32)).astype(BF)
        q_s2[k, 0, pl.ds(32, 32), :] = q_part[k, at(1, 32, 32), :].astype(BF)
        send(q_s2.at[k, 0], q_r2.at[k, 0], ("r2", k, 0), up_y)
        arrive(q_r1.at[k, 1], ("r1", k, 1), up_y)
        q_s2[k, 1, pl.ds(0, 32), :] = q_part[k, at(3, 0, 32), :].astype(BF)
        q_s2[k, 1, pl.ds(32, 32), :] = (q_part[k, at(3, 32, 32), :] + q_r1[k, 1].astype(F32)).astype(BF)
        send(q_s2.at[k, 1], q_r2.at[k, 1], ("r2", k, 1), dn_y)

    def q_sum(k):
        arrive(q_r2.at[k, 0], ("r2", k, 0), dn_y)
        arrive(q_r2.at[k, 1], ("r2", k, 1), up_y)
        at = pl.ds(pl.multiple_of(y * 64, 64), 64)
        return q_part[k, at, :] + q_r2[k, 0].astype(F32) + q_r2[k, 1].astype(F32)

    def q_leave(k):
        q_s3[k - 1] = q_sum(k).astype(BF)
        send(q_s3.at[k - 1], q_r3.at[k - 1], ("r3", k), {"zl": planes[k]})

    def q_end():
        total = q_sum(0)
        for k in (1, 2, 3):
            arrive(q_r3.at[k - 1], ("r3", k), {"zl": planes[k]})
            total = total + q_r3[k - 1].astype(F32)
        qg_ref[...] = total.astype(BF)

    steps = [
        (slopes, 0), (c_dot, 0), (slopes, 1), (slopes_mate, 0), (slopes_mate, 1), (q_dot, 1), (c_mid, 0), (q_dot, 2),
        (q_mid, 1), (q_dot, 3), (c_dot, 1), (q_mid, 2), (q_leave, 1), (c_leave,), (q_dot, 0), (q_mid, 3), (c_mid, 1),
        (q_leave, 2), (q_mid, 0), (q_leave, 3), (c_pass,), (q_end,), (c_end,),
    ]
    for step, *given in steps:
        step(*given)
    wires.finish()


def local(queries, candidates, grades, query_weights):
    vmem = pl.BlockSpec(memory_space=pltpu.VMEM)
    weights = query_weights.reshape(16, LANES)
    shapes = [
        ((2048, 1024), BF), ((1024, 1024), BF), ((1024, 1024), BF), ((16, LANES), F32), ((4, 128, 1024), jnp.int32),
        ((1024, 2048), jnp.int32), ((1024, 2048), F32), ((1024, 2048), BF), ((1024, 1024), BF),
        ((2, 64, 1024), BF), ((2, 16, 8, LANES), F32), ((2, 16, 16, LANES), F32), ((16, 16, LANES), F32),
        ((16, 16, LANES), F32), ((2, 16, LANES), F32), ((16, 16, LANES), F32),
        ((4, 256, 1024), F32), ((4, 2, 32, 1024), BF), ((4, 2, 32, 1024), BF), ((4, 2, 64, 1024), BF),
        ((4, 2, 64, 1024), BF), ((3, 64, 1024), BF), ((3, 64, 1024), BF),
        ((2, 512, 1024), F32), ((2, 2, 64, 1024), BF), ((2, 2, 64, 1024), BF), ((2, 2, 128, 1024), BF),
        ((2, 2, 128, 1024), BF), ((128, 1024), BF), ((2, 64, 1024), BF), ((128, 1024), BF),
    ]
    losses, query_grad, cand_grad = pl.pallas_call(
        kernel,
        out_shape=(
            jax.ShapeDtypeStruct((16, LANES), F32),
            jax.ShapeDtypeStruct((64, 1024), BF),
            jax.ShapeDtypeStruct((128, 1024), BF),
        ),
        in_specs=[vmem, vmem, vmem, pl.BlockSpec(memory_space=pl.ANY)],
        out_specs=(vmem, vmem, vmem),
        scratch_shapes=[pltpu.VMEM(shape, dtype) for shape, dtype in shapes]
        + [
            pltpu.SemaphoreType.DMA((160,)),
            pltpu.SemaphoreType.DMA((160,)),
            pltpu.SemaphoreType.DMA((4, 2)),
        ],
        compiler_params=pltpu.CompilerParams(
            collective_id=0, has_side_effects=True, vmem_limit_bytes=66 * 1000 * 1000
        ),
        name="listmle",
    )(queries, candidates, weights, grades)
    return losses.reshape(2048), query_grad, cand_grad


def solution(mesh):
    split = Mesh(mesh.devices.reshape(2, 4, 4, 4, 2), AXES)
    return jax.shard_map(
        local,
        mesh=split,
        in_specs=(P(AXES_Q := ROWS + COL, None), P(COL + ROWS, None), P(ROWS, COL), P(ROWS)),
        out_specs=(P(ROWS), P(AXES_Q, None), P(COL + ROWS, None)),
        check_vma=False,
    )
```

```python
import jax
import jax.numpy as jnp
from jax import lax
from jax.experimental import pallas as pl
from jax.experimental.pallas import tpu as pltpu
from jax.sharding import Mesh
from jax.sharding import PartitionSpec as P

GRADES = 5
LOWEST = -1e30
AXES = ("zh", "x", "y", "zl", "c")
ROWS = ("zh", "x")
COL = ("y", "zl", "c")
SCALE = 1.0 / 32.0
EXP2_SCALE = 1.4426950408889634 / 32.0
BF = jnp.bfloat16
F32 = jnp.float32
LANES = 128


class Wires:
    def __init__(self, send_sems, recv_sems):
        self.send_sems, self.recv_sems = send_sems, recv_sems
        self.names, self.sent = {}, []

    def slot(self, name):
        return self.names.setdefault(name, len(self.names))

    def send(self, src, dst, name, where):
        copy = pltpu.make_async_remote_copy(
            src_ref=src,
            dst_ref=dst,
            send_sem=self.send_sems.at[len(self.sent)],
            recv_sem=self.recv_sems.at[self.slot(name)],
            device_id=where,
            device_id_type=pl.DeviceIdType.MESH,
        )
        copy.start()
        self.sent.append(copy)

    def arrive(self, dst, name, where):
        pltpu.make_async_remote_copy(
            src_ref=dst,
            dst_ref=dst,
            send_sem=self.send_sems.at[0],
            recv_sem=self.recv_sems.at[self.slot(name)],
            device_id=where,
            device_id_type=pl.DeviceIdType.MESH,
        ).wait_recv()

    def finish(self):
        for copy in self.sent:
            copy.wait_send()


def combine(parts):
    row = lax.broadcasted_iota(jnp.int32, (8, LANES), 0)
    stat = row < GRADES
    top = parts[0][0]
    for first, _ in parts[1:]:
        top = jnp.maximum(top, first)
    plain = jnp.zeros((8, LANES), F32)
    mass = jnp.zeros((8, LANES), F32)
    for first, second in parts:
        plain = plain + first
        mass = mass + second * jnp.where(stat, jnp.exp(first - top), 1.0)
    return jnp.where(stat, top, plain), mass


def stacked(rows):
    row = lax.broadcasted_iota(jnp.int32, (8, LANES), 0)
    out = jnp.zeros((8, LANES), F32)
    for k, value in enumerate(rows):
        out = jnp.where(row == k, value, out)
    return out


def outcome(first, second, columns):
    maxima = [first[k : k + 1] for k in range(GRADES)]
    masses = [second[k : k + 1] for k in range(GRADES)]
    counts = [first[5:6], first[6:7], first[7:8], second[5:6], second[6:7]]
    totals = second[7:8]
    levels, running, seen = [], maxima[0], jnp.zeros_like(totals)
    for k in range(GRADES):
        running = jnp.maximum(running, maxima[k])
        seen = seen + counts[k]
        summed = masses[0] * jnp.exp(maxima[0] - running)
        for h in range(1, k + 1):
            summed = summed + masses[h] * jnp.exp(maxima[h] - running)
        present = seen > 0.0
        levels.append(jnp.where(present, running + jnp.log(jnp.where(present, summed, 1.0)), running))
    weighted = counts[0] * levels[0]
    for k in range(1, GRADES):
        weighted = weighted + counts[k] * levels[k]
    losses = (weighted - totals) / columns
    factors = []
    for h in range(GRADES):
        summed = counts[h] * jnp.exp(maxima[h] - levels[h])
        for k in range(h + 1, GRADES):
            summed = summed + counts[k] * jnp.exp(maxima[h] - levels[k])
        factors.append(summed)
    return stacked(maxima), stacked(factors + [losses])


GATHER = lax.GatherDimensionNumbers(
    offset_dims=(),
    collapsed_slice_dims=(0,),
    start_index_map=(0,),
    operand_batching_dims=(1,),
    start_indices_batching_dims=(1,),
)


def spread(table, grade):
    pieces = [
        lax.gather(
            table,
            grade[at : at + 8][..., None],
            GATHER,
            slice_sizes=(1, 1),
            mode=lax.GatherScatterMode.PROMISE_IN_BOUNDS,
        )
        for at in range(0, grade.shape[0], 8)
    ]
    return jnp.concatenate(pieces, axis=0)


def folded(op, block):
    return op(block.reshape(-1, 8, LANES), axis=0)


def kernel(
    q_hbm, c_hbm, w_hbm, g_hbm, loss_ref, qg_ref, cg_ref,
    q_all, c_all, c_par, w_ref, w_t, g_in, g_t, es, sl, sl_par, z_rel, cnt, st_half, st, st_in, st_core, res,
    q_part, q_s1, q_r1, q_s2, q_r2, q_s3, q_r3,
    c_part, c_s1, c_r1, c_s2, c_r2, c_s3, c_rel, c_r3,
    send_sems, recv_sems, g_sems, in_sems,
):
    zh, x, y, zl, c = (lax.axis_index(a) for a in AXES)
    other = 1 - c
    wires = Wires(send_sems, recv_sems)
    send, arrive = wires.send, wires.arrive
    up_y, dn_y = {"y": (y + 1) % 4}, {"y": (y + 3) % 4}
    up_x, dn_x = {"x": (x + 1) % 4}, {"x": (x + 3) % 4}
    mate = {"c": other}
    zl2 = (zl + 2) % 4
    planes = (zl, zl + 1 - 2 * (zl % 2), zl2, 3 - zl)
    up_zh, dn_zh = (zh + zl // 2) % 2, (zh + 1 + zl // 2) % 2
    up_z, dn_z = {"zh": up_zh, "zl": zl2}, {"zh": dn_zh, "zl": zl2}

    def q_rows(core, k, dy, start=0, size=64):
        at = core * 1024 + planes[k] * 256 + (y + dy) % 4 * 64 + start
        return q_all.at[pl.ds(pl.multiple_of(at, 32), size), :]

    def c_rows(half, dx, start=0, size=128):
        at = half * 512 + (x + dx) % 4 * 128 + start
        return c_all.at[pl.ds(pl.multiple_of(at, 32), size), :]

    own = [
        pltpu.make_async_copy(q_hbm, q_rows(c, 0, 0), in_sems.at[0]),
        pltpu.make_async_copy(c_hbm, c_rows(zh, 0), in_sems.at[1]),
        pltpu.make_async_copy(w_hbm, w_ref, in_sems.at[2]),
    ]
    for copy in own:
        copy.start()

    def grade_copies(tile):
        core, plane, pair = tile // 8, tile // 2 % 4, tile % 2
        copies = []
        for i in range(2):
            at = (((pair * 2 + i) * 4 + plane) * 2 + core) * 64
            copies.append(
                pltpu.make_async_copy(
                    g_hbm.at[pl.ds(at, 64), :],
                    g_in.at[tile % 4, pl.ds(64 * i, 64), :],
                    g_sems.at[tile % 4, i],
                )
            )
        return copies

    for tile in range(4):
        for copy in grade_copies(tile):
            copy.start()

    barrier = pltpu.get_barrier_semaphore()
    greeted = [{"zl": planes[k]} for k in (1, 2, 3)] + [up_y, dn_y, up_x, dn_x, mate, {"zh": 1 - zh, "zl": zl2}]
    for device in greeted:
        pl.semaphore_signal(barrier, inc=1, device_id=device, device_id_type=pl.DeviceIdType.MESH)
    pl.semaphore_wait(barrier, len(greeted))

    for copy in own:
        copy.wait()
    q_own, c_own = q_rows(c, 0, 0), c_rows(zh, 0)
    for i in range(2):
        for h, where in ((0, up_z), (1, dn_z)):
            send(c_rows(zh, 0, 64 * h + 32 * i, 32), z_rel.at[h, pl.ds(32 * i, 32), :], ("zr", h, i), where)
    send(q_own, q_own, ("qy", 0, 0), up_y)
    send(q_own, q_own, ("qy", 0, 1), dn_y)
    send(c_own, c_own, ("cx", 0), up_x)
    send(c_own, c_own, ("cx", 1), dn_x)
    send(q_own, q_own, ("qz", 2), {"zl": planes[2]})
    send(q_own, q_own, ("qd", 0, 0), mate)
    for t in range(16):
        core, at = t // 8, t % 2 * 8 + t // 2 % 4
        pair = [w_ref[pl.ds(at, 1), :], w_ref[pl.ds(at + 4, 1), :]]
        pair[1 - core] = pltpu.roll(pair[1 - core], 64, 1)
        w_t[pl.ds(t, 1), :] = jnp.where(lax.broadcasted_iota(jnp.int32, (1, LANES), 1) < 64, *pair)

    def to_mate(k, dy):
        send(q_rows(c, k, dy), q_rows(c, k, dy), ("qd", k, dy), mate)

    def q_near(k):
        arrive(q_rows(c, k, 3), ("qy", k, 0), dn_y)
        send(q_rows(c, k, 3, 0, 32), q_rows(c, k, 3, 0, 32), ("qf", k, 0), up_y)
        to_mate(k, 3)
        arrive(q_rows(c, k, 1), ("qy", k, 1), up_y)
        send(q_rows(c, k, 1, 32, 32), q_rows(c, k, 1, 32, 32), ("qf", k, 1), dn_y)
        to_mate(k, 1)

    def q_far(k):
        arrive(q_rows(c, k, 2, 0, 32), ("qf", k, 0), dn_y)
        arrive(q_rows(c, k, 2, 32, 32), ("qf", k, 1), up_y)
        to_mate(k, 2)

    def q_over(k):
        arrive(q_rows(c, k, 0), ("qz", k), {"zl": planes[k if k < 3 else 1]})
        send(q_rows(c, k, 0), q_rows(c, k, 0), ("qy", k, 0), up_y)
        send(q_rows(c, k, 0), q_rows(c, k, 0), ("qy", k, 1), dn_y)
        if k == 2:
            send(q_rows(c, k, 0), q_rows(c, k, 0), ("qz", 3), {"zl": planes[1]})
        to_mate(k, 0)

    def c_near():
        arrive(c_rows(zh, 3), ("cx", 0), dn_x)
        send(c_rows(zh, 3, 0, 64), c_rows(zh, 3, 0, 64), ("cf", 0), up_x)
        arrive(c_rows(zh, 1), ("cx", 1), up_x)
        send(c_rows(zh, 1, 64, 64), c_rows(zh, 1, 64, 64), ("cf", 1), dn_x)

    def c_far():
        arrive(c_rows(zh, 2, 0, 64), ("cf", 0), dn_x)
        arrive(c_rows(zh, 2, 64, 64), ("cf", 1), up_x)

    def c_relay(i):
        for h, frm, where, there in ((0, dn_z, up_z, up_zh), (1, up_z, dn_z, dn_zh)):
            part = z_rel.at[h, pl.ds(32 * i, 32), :]
            arrive(part, ("zr", h, i), frm)
            send(part, c_rows(1 - there, 0, 64 * h + 32 * i, 32), ("cz", h, i), where)

    def q_leap():
        send(q_own, q_own, ("qz", 1), {"zl": planes[1]})

    def c_over(i):
        for h, frm in ((0, dn_z), (1, up_z)):
            part = c_rows(1 - zh, 0, 64 * h + 32 * i, 32)
            arrive(part, ("cz", h, i), frm)
            send(part, part, ("px", h, i, 0), up_x)
            send(part, part, ("px", h, i, 1), dn_x)

    def p_near(i):
        for h in range(2):
            below, above = c_rows(1 - zh, 3, 64 * h + 32 * i, 32), c_rows(1 - zh, 1, 64 * h + 32 * i, 32)
            arrive(below, ("px", h, i, 0), dn_x)
            if h == 0:
                send(below, below, ("pf", 0, i), up_x)
            arrive(above, ("px", h, i, 1), up_x)
            if h == 1:
                send(above, above, ("pf", 1, i), dn_x)

    def p_far():
        for i in range(2):
            for h, frm in ((0, dn_x), (1, up_x)):
                arrive(c_rows(1 - zh, 2, 64 * h + 32 * i, 32), ("pf", h, i), frm)

    def turn(tile):
        for copy in grade_copies(tile):
            copy.wait()
        for b in range(8):
            block = g_in[tile % 4, :, pl.ds(128 * b, 128)]
            g_t[pl.ds(128 * b, 128), pl.ds(128 * tile, 128)] = jnp.transpose(block)
        if tile + 4 < 16:
            for copy in grade_copies(tile + 4):
                copy.start()

        for h in range(2):

            def tally(i, held):
                at = pl.ds(pl.multiple_of(h * 512 + i * 64, 64), 64)
                grade = g_t[at, pl.ds(128 * tile, 128)]
                return tuple(v + folded(jnp.sum, jnp.where(grade == k, 1.0, 0.0)) for k, v in enumerate(held))

            held = lax.fori_loop(0, 8, tally, (jnp.zeros((8, LANES), F32),) * 4)
            held = [jnp.sum(v, axis=0, keepdims=True) for v in held]
            held.append(512.0 - (held[0] + held[1] + held[2] + held[3]))
            cnt[h, tile] = stacked(held)

    def pair_stats(half, first):
        lanes = [pl.ds(pl.multiple_of((first + i) * LANES, LANES), LANES) for i in range(2)]
        zero = jnp.zeros((8, LANES), F32)
        low = jnp.full((8, LANES), 32.0 * LOWEST, F32)

        def highest(n, held):
            at = pl.ds(pl.multiple_of(half * 512 + n * 64, 64), 64)
            new = []
            for i in range(2):
                score, grade = es[at, lanes[i]], g_t[at, lanes[i]]
                for k in range(GRADES):
                    found = folded(jnp.max, jnp.where(grade == k, score, 32.0 * LOWEST))
                    new.append(jnp.maximum(held[6 * i + k], found))
                new.append(held[6 * i + GRADES] + folded(jnp.sum, score))
            return tuple(new)

        held = lax.fori_loop(0, 8, highest, ((low,) * GRADES + (zero,)) * 2)
        maxima = [[jnp.max(v, axis=0, keepdims=True) for v in held[6 * i : 6 * i + GRADES]] for i in range(2)]
        total = [jnp.sum(held[6 * i + GRADES], axis=0, keepdims=True) * SCALE for i in range(2)]
        tables = [stacked(m) for m in maxima]

        def masses_of(n, held):
            at = pl.ds(pl.multiple_of(half * 512 + n * 64, 64), 64)
            new, values = [], []
            for i in range(2):
                score, grade = es[at, lanes[i]], g_t[at, lanes[i]]
                value = jnp.exp2((score - spread(tables[i], grade)) * EXP2_SCALE)
                values.append(value)
                for k in range(GRADES):
                    new.append(held[5 * i + k] + folded(jnp.sum, jnp.where(grade == k, value, 0.0)))
            for i in range(2):
                es[at, lanes[i]] = values[i]
            return tuple(new)

        held = lax.fori_loop(0, 8, masses_of, (zero,) * (2 * GRADES))
        for i in range(2):
            masses = [jnp.sum(v, axis=0, keepdims=True) for v in held[5 * i : 5 * i + GRADES]]
            counts = [cnt[half, first + i, pl.ds(k, 1), :] for k in range(GRADES)]
            st_half[half, first + i, pl.ds(0, 8), :] = stacked([m * SCALE for m in maxima[i]] + counts[:3])
            st_half[half, first + i, pl.ds(8, 8), :] = stacked(masses + counts[3:] + [total[i]])

    def unit(h, k):
        half = (zh + h) % 2
        cands = pl.ds(pl.multiple_of(half * 512, 512), 512)

        def one(core, _):
            n = core * 4 + planes[k]
            rows = pl.ds(pl.multiple_of(n * 256, 256), 256)
            es[cands, rows] = lax.dot_general(
                c_all[cands, :], q_all[rows, :], (((1,), (1,)), ((), ())), preferred_element_type=F32
            )
            pair_stats(half, 2 * n)
            return 0

        lax.fori_loop(0, 2, one, 0)

    columns = (y, y + 1 - 2 * (y % 2), (y + 2) % 4, 3 - y)
    slots = [(d, k) for k in range(4) for d in range(4)]

    def tile_of(d, k):
        return columns[d] // 2 * 8 + planes[k] * 2 + columns[d] % 2

    def chip(d, k):
        return {"y": columns[d], "zl": planes[k]}

    def st_out(k):
        for d in range(4):
            t, n = tile_of(d, k), k * 4 + d
            first, second = combine(
                [(st_half[h, t, pl.ds(0, 8), :], st_half[h, t, pl.ds(8, 8), :]) for h in range(2)]
            )
            st[n, pl.ds(0, 8), :] = first
            st[n, pl.ds(8, 8), :] = second
        for d in range(4):
            if (d, k) != (0, 0):
                n = k * 4 + d
                send(st.at[n], st_in.at[n], ("st", d, k), chip(d, k))

    def turns(first, last):
        for tile in range(first, last):
            turn(tile)

    def q_mate(k):
        for dy in range(4):
            arrive(q_rows(other, k, dy), ("qd", k, dy), mate)

    steps = [
        (turns, 0, 6), (q_near, 0), (c_relay, 0), (turns, 6, 8), (c_near,), (c_relay, 1), (q_leap,), (turns, 8, 11),
        (q_over, 2), (q_far, 0), (c_far,), (turns, 11, 13), (c_over, 0), (turns, 13, 16), (q_mate, 0), (c_over, 1), (q_near, 2),
        (p_near, 0), (q_over, 1), (unit, 0, 0), (p_near, 1), (q_over, 3), (q_far, 2), (q_mate, 2), (unit, 0, 2), (q_near, 1),
        (p_far,), (send, c_all, c_par, ("cp",), mate), (q_near, 3), (unit, 1, 0), (st_out, 0), (q_far, 1), (unit, 1, 2),
        (st_out, 2), (q_mate, 1), (q_far, 3), (unit, 0, 1), (unit, 1, 1), (st_out, 1), (q_mate, 3), (unit, 0, 3), (unit, 1, 3),
        (st_out, 3),
    ]
    for step, *given in steps:
        step(*given)

    mine = tile_of(0, 0)
    parts = [(st[0, pl.ds(0, 8), :], st[0, pl.ds(8, 8), :])]
    for d, k in slots[1:]:
        n = k * 4 + d
        arrive(st_in.at[n], ("st", d, k), chip(d, k))
        parts.append((st_in[n, pl.ds(0, 8), :], st_in[n, pl.ds(8, 8), :]))
    first, second = combine(parts)
    st_core[0, pl.ds(0, 8), :] = first
    st_core[0, pl.ds(8, 8), :] = second
    send(st_core.at[0], st_core.at[1], ("sd",), mate)
    arrive(st_core.at[1], ("sd",), mate)
    first, second = combine([(first, second), (st_core[1, pl.ds(0, 8), :], st_core[1, pl.ds(8, 8), :])])
    first, second = outcome(first, second, 32768.0)
    res[mine, pl.ds(0, 8), :] = first
    res[mine, pl.ds(8, 8), :] = second
    for d, k in reversed(slots[1:]):
        send(res.at[mine], res.at[mine], ("sr", d, k), chip(d, k))
    arrive(c_par, ("cp",), mate)
    for d, k in slots[1:]:
        arrive(res.at[tile_of(d, k)], ("sr", d, k), chip(d, k))
    found = [res[t, pl.ds(13, 1), :] for t in range(16)]
    low_lanes = lax.broadcasted_iota(jnp.int32, (1, LANES), 1) < 64
    for v in range(4):
        for p in range(4):
            pair = [found[core * 8 + p * 2 + v // 2] for core in range(2)]
            pair[1 - v % 2] = pltpu.roll(pair[1 - v % 2], 64, 1)
            loss_ref[pl.ds(v * 4 + p, 1), :] = jnp.where(low_lanes, pair[0], pair[1])

    row = lax.broadcasted_iota(jnp.int32, (8, LANES), 0)
    for t in range(16):
        weight = w_t[pl.ds(t, 1), :] * SCALE
        for h in range(2):
            table = res[t, pl.ds(8, 8), :] * jnp.exp(st_half[h, t, pl.ds(0, 8), :] - res[t, pl.ds(0, 8), :])
            table = jnp.where(row < GRADES, table, 0.0) * weight
            st_half[h, t, pl.ds(8, 8), :] = jnp.where(row == 7, weight, table)

    def slope_block(j, d):
        half = (zh + 1 - j) % 2
        at = pl.ds(pl.multiple_of(half * 512 + (x + d) % 4 * 128, 128), 128)

        def one(t, _):
            lanes = pl.ds(pl.multiple_of(t * LANES, LANES), LANES)
            table = st_half[half, t, pl.ds(8, 8), :]
            sl[at, lanes] = (spread(table, g_t[at, lanes]) * es[at, lanes] - table[7:8]).astype(BF)
            return 0

        lax.fori_loop(0, 16, one, 0)

    def slopes_out(j):
        cands = pl.ds(pl.multiple_of((zh + 1 - j) % 2 * 512, 512), 512)
        send(sl.at[cands, pl.ds(pl.multiple_of(other * 1024, 1024), 1024)], sl_par.at[cands, :], ("sl", j), mate)

    def lanes_of(core, plane):
        return pl.ds(pl.multiple_of(core * 1024 + plane * 256, 256), 256)

    def slopes_mate(j):
        cands = pl.ds(pl.multiple_of((zh + 1 - j) % 2 * 512, 512), 512)
        arrive(sl_par.at[cands, :], ("sl", j), mate)

    def c_block(d, start=0, size=128):
        return pl.ds(pl.multiple_of((x + d) % 4 * 128 + start, 32), size)

    def c_dot(j, d):
        at = pl.multiple_of((zh + 1 - j) % 2 * 512 + (x + d) % 4 * 128, 128)
        c_part[j, c_block(d), :] = jnp.dot(sl[pl.ds(at, 128), :], q_all[...], preferred_element_type=F32)

    def c_far_part(j):
        c_dot(j, 2)
        for side in range(2):
            c_s1[j, side] = c_part[j, c_block(2, 64 * side, 64), :].astype(BF)
        for i in range(2):
            for side, where in ((0, up_x), (1, dn_x)):
                at = pl.ds(32 * i, 32)
                send(c_s1.at[j, side, at, :], c_r1.at[j, side, at, :], ("s1", j, side, i), where)

    def c_rest(j):
        for d, side in ((1, 0), (3, 1)):
            c_dot(j, d)
            at = pl.ds(64 - 64 * side, 64)
            c_s2[j, side, at, :] = c_part[j, c_block(d, 64 - 64 * side, 64), :].astype(BF)
        for i in range(2):
            for side, where in ((0, up_x), (1, dn_x)):
                at = pl.ds(64 - 64 * side + 32 * i, 32)
                send(c_s2.at[j, side, at, :], c_r2.at[j, side, at, :], ("s2", j, side, i), where)

    def c_mid(j, i):
        for d, side, frm, where in ((1, 0, dn_x, up_x), (3, 1, up_x, dn_x)):
            half = pl.ds(32 * i, 32)
            arrive(c_r1.at[j, side, half, :], ("s1", j, side, i), frm)
            at = pl.ds(64 * side + 32 * i, 32)
            own_part = c_part[j, c_block(d, 64 * side + 32 * i, 32), :]
            c_s2[j, side, at, :] = (own_part + c_r1[j, side, half, :].astype(F32)).astype(BF)
            send(c_s2.at[j, side, at, :], c_r2.at[j, side, at, :], ("s4", j, side, i), where)

    def c_take(j, i):
        for side, frm in ((0, dn_x), (1, up_x)):
            arrive(c_r2.at[j, side, pl.ds(64 - 64 * side + 32 * i, 32), :], ("s2", j, side, i), frm)
            arrive(c_r2.at[j, side, pl.ds(64 * side + 32 * i, 32), :], ("s4", j, side, i), frm)

    def c_leave(i):
        c_take(0, i)
        for h, where in ((0, up_z), (1, dn_z)):
            at = pl.ds(64 * h + 32 * i, 32)
            total = c_part[0, c_block(0, 64 * h + 32 * i, 32), :] + c_r2[0, 0, at, :].astype(F32) + c_r2[0, 1, at, :].astype(F32)
            c_s3[at, :] = total.astype(BF)
            send(c_s3.at[at, :], c_rel.at[h, pl.ds(32 * i, 32), :], ("t1", h, i), where)

    def c_pass(i):
        for h, frm, where in ((0, dn_z, up_z), (1, up_z, dn_z)):
            part = c_rel.at[h, pl.ds(32 * i, 32), :]
            arrive(part, ("t1", h, i), frm)
            send(part, c_r3.at[pl.ds(64 * h + 32 * i, 32), :], ("t2", h, i), where)

    def c_end():
        for i in range(2):
            c_take(1, i)
        total = c_part[1, c_block(0), :] + c_r2[1, 0].astype(F32) + c_r2[1, 1].astype(F32)
        for i in range(2):
            for h, frm in ((0, dn_z), (1, up_z)):
                arrive(c_r3.at[pl.ds(64 * h + 32 * i, 32), :], ("t2", h, i), frm)
        cg_ref[...] = (total + c_r3[...].astype(F32)).astype(BF)

    dims = (((0,), (0,)), ((), ()))

    def q_block(d, start, size):
        return pl.ds(pl.multiple_of((y + d) % 4 * 64 + start, 32), size)

    def q_dot(k):
        plane = planes[k]
        q_part[k] = lax.dot_general(
            sl[:, lanes_of(c, plane)], c_all[...], dims, preferred_element_type=F32
        ) + lax.dot_general(sl_par[:, lanes_of(0, plane)], c_par[...], dims, preferred_element_type=F32)

        q_s1[k, 0] = q_part[k, q_block(2, 0, 32), :].astype(BF)
        q_s1[k, 1] = q_part[k, q_block(2, 32, 32), :].astype(BF)
        send(q_s1.at[k, 0], q_r1.at[k, 0], ("r1", k, 0), up_y)
        send(q_s1.at[k, 1], q_r1.at[k, 1], ("r1", k, 1), dn_y)
        for d, side, where in ((1, 0, up_y), (3, 1, dn_y)):
            at = pl.ds(32 - 32 * side, 32)
            q_s2[k, side, at, :] = q_part[k, q_block(d, 32 - 32 * side, 32), :].astype(BF)
            send(q_s2.at[k, side, at, :], q_r2.at[k, side, at, :], ("r2", k, side), where)

    def q_mid(k):
        for d, side, frm, where in ((1, 0, dn_y, up_y), (3, 1, up_y, dn_y)):
            arrive(q_r1.at[k, side], ("r1", k, side), frm)
            at = pl.ds(32 * side, 32)
            q_s2[k, side, at, :] = (q_part[k, q_block(d, 32 * side, 32), :] + q_r1[k, side].astype(F32)).astype(BF)
            send(q_s2.at[k, side, at, :], q_r2.at[k, side, at, :], ("r4", k, side), where)

    def q_sum(k):
        for side, frm in ((0, dn_y), (1, up_y)):
            arrive(q_r2.at[k, side, pl.ds(32 - 32 * side, 32), :], ("r2", k, side), frm)
            arrive(q_r2.at[k, side, pl.ds(32 * side, 32), :], ("r4", k, side), frm)
        at = pl.ds(pl.multiple_of(y * 64, 64), 64)
        return q_part[k, at, :] + q_r2[k, 0].astype(F32) + q_r2[k, 1].astype(F32)

    def q_leave(k):
        total = q_sum(k)
        if k == 2:
            arrive(q_r3.at[2], ("r3", 3), {"zl": planes[1]})
            total = total + q_r3[2].astype(F32)
        q_s3[k - 1] = total.astype(BF)
        send(q_s3.at[k - 1], q_r3.at[k - 1], ("r3", k), {"zl": planes[k if k < 3 else 1]})

    def q_end():
        total = q_sum(0)
        for k in (1, 2):
            arrive(q_r3.at[k - 1], ("r3", k), {"zl": planes[k]})
            total = total + q_r3[k - 1].astype(F32)
        qg_ref[...] = total.astype(BF)

    steps = [
        (slope_block, 0, 2), (c_far_part, 0), (slope_block, 0, 1), (slope_block, 0, 3), (c_rest, 0), (slope_block, 0, 0),
        (slopes_out, 0), (c_mid, 0, 0), (slope_block, 1, 0), (slope_block, 1, 1), (slope_block, 1, 2), (slope_block, 1, 3),
        (slopes_out, 1), (c_mid, 0, 1), (c_dot, 0, 0), (slopes_mate, 0), (slopes_mate, 1), (q_dot, 3), (c_leave, 0), (q_dot, 2),
        (q_mid, 3), (c_leave, 1), (q_dot, 1), (c_pass, 0), (q_mid, 2), (q_leave, 3), (c_pass, 1), (q_mid, 1), (c_far_part, 1),
        (c_rest, 1), (q_leave, 2), (q_dot, 0), (q_leave, 1), (c_mid, 1, 0), (c_mid, 1, 1), (c_dot, 1, 0), (q_mid, 0), (q_end,),
        (c_end,),
    ]
    for step, *given in steps:
        step(*given)
    wires.finish()


def local(queries, candidates, grades, query_weights):
    vmem = pl.BlockSpec(memory_space=pltpu.VMEM)
    weights = query_weights.reshape(16, LANES)
    shapes = [
        ((2048, 1024), BF), ((1024, 1024), BF), ((1024, 1024), BF), ((16, LANES), F32), ((16, LANES), F32), ((4, 128, 1024), jnp.int32),
        ((1024, 2048), jnp.int32), ((1024, 2048), F32), ((1024, 2048), BF), ((1024, 1024), BF),
        ((2, 64, 1024), BF), ((2, 16, 8, LANES), F32), ((2, 16, 16, LANES), F32), ((16, 16, LANES), F32),
        ((16, 16, LANES), F32), ((2, 16, LANES), F32), ((16, 16, LANES), F32),
        ((4, 256, 1024), F32), ((4, 2, 32, 1024), BF), ((4, 2, 32, 1024), BF), ((4, 2, 64, 1024), BF),
        ((4, 2, 64, 1024), BF), ((3, 64, 1024), BF), ((3, 64, 1024), BF),
        ((2, 512, 1024), F32), ((2, 2, 64, 1024), BF), ((2, 2, 64, 1024), BF), ((2, 2, 128, 1024), BF),
        ((2, 2, 128, 1024), BF), ((128, 1024), BF), ((2, 64, 1024), BF), ((128, 1024), BF),
    ]
    losses, query_grad, cand_grad = pl.pallas_call(
        kernel,
        out_shape=(
            jax.ShapeDtypeStruct((16, LANES), F32),
            jax.ShapeDtypeStruct((64, 1024), BF),
            jax.ShapeDtypeStruct((128, 1024), BF),
        ),
        in_specs=[pl.BlockSpec(memory_space=pl.ANY)] * 4,
        out_specs=(vmem, vmem, vmem),
        scratch_shapes=[pltpu.VMEM(shape, dtype) for shape, dtype in shapes]
        + [
            pltpu.SemaphoreType.DMA((192,)),
            pltpu.SemaphoreType.DMA((192,)),
            pltpu.SemaphoreType.DMA((4, 2)),
            pltpu.SemaphoreType.DMA((3,)),
        ],
        compiler_params=pltpu.CompilerParams(
            collective_id=0, has_side_effects=True, vmem_limit_bytes=66 * 1000 * 1000
        ),
        name="listmle",
    )(queries, candidates, weights, grades)
    return losses.reshape(2048), query_grad, cand_grad


def solution(mesh):
    split = Mesh(mesh.devices.reshape(2, 4, 4, 4, 2), AXES)
    return jax.shard_map(
        local,
        mesh=split,
        in_specs=(P(AXES_Q := ROWS + COL, None), P(COL + ROWS, None), P(ROWS, COL), P(ROWS)),
        out_specs=(P(ROWS), P(AXES_Q, None), P(COL + ROWS, None)),
        check_vma=False,
    )
```

```python
import jax
import jax.numpy as jnp
from jax import lax
from jax.experimental import pallas as pl
from jax.experimental.pallas import tpu as pltpu
from jax.sharding import Mesh
from jax.sharding import PartitionSpec as P

GRADES = 5
LOWEST = -1e30
AXES = ("zh", "x", "y", "zl", "c")
ROWS = ("zh", "x")
COL = ("y", "zl", "c")
SCALE = 1.0 / 32.0
EXP2_SCALE = 1.4426950408889634 / 32.0
BF = jnp.bfloat16
F32 = jnp.float32
LANES = 128


class Wires:
    def __init__(self, send_sems, recv_sems):
        self.send_sems, self.recv_sems = send_sems, recv_sems
        self.names, self.sent = {}, []

    def slot(self, name):
        return self.names.setdefault(name, len(self.names))

    def send(self, src, dst, name, where):
        copy = pltpu.make_async_remote_copy(
            src_ref=src,
            dst_ref=dst,
            send_sem=self.send_sems.at[len(self.sent)],
            recv_sem=self.recv_sems.at[self.slot(name)],
            device_id=where,
            device_id_type=pl.DeviceIdType.MESH,
        )
        copy.start()
        self.sent.append(copy)

    def arrive(self, dst, name, where):
        pltpu.make_async_remote_copy(
            src_ref=dst,
            dst_ref=dst,
            send_sem=self.send_sems.at[0],
            recv_sem=self.recv_sems.at[self.slot(name)],
            device_id=where,
            device_id_type=pl.DeviceIdType.MESH,
        ).wait_recv()

    def finish(self):
        for copy in self.sent:
            copy.wait_send()


def combine(parts):
    row = lax.broadcasted_iota(jnp.int32, (8, LANES), 0)
    stat = row < GRADES
    top = parts[0][0]
    for first, _ in parts[1:]:
        top = jnp.maximum(top, first)
    plain = jnp.zeros((8, LANES), F32)
    mass = jnp.zeros((8, LANES), F32)
    for first, second in parts:
        plain = plain + first
        mass = mass + second * jnp.where(stat, jnp.exp(first - top), 1.0)
    return jnp.where(stat, top, plain), mass


def stacked(rows):
    row = lax.broadcasted_iota(jnp.int32, (8, LANES), 0)
    out = jnp.zeros((8, LANES), F32)
    for k, value in enumerate(rows):
        out = jnp.where(row == k, value, out)
    return out


def outcome(first, second, columns):
    maxima = [first[k : k + 1] for k in range(GRADES)]
    masses = [second[k : k + 1] for k in range(GRADES)]
    counts = [first[5:6], first[6:7], first[7:8], second[5:6], second[6:7]]
    totals = second[7:8]
    levels, running, seen = [], maxima[0], jnp.zeros_like(totals)
    for k in range(GRADES):
        running = jnp.maximum(running, maxima[k])
        seen = seen + counts[k]
        summed = masses[0] * jnp.exp(maxima[0] - running)
        for h in range(1, k + 1):
            summed = summed + masses[h] * jnp.exp(maxima[h] - running)
        present = seen > 0.0
        levels.append(jnp.where(present, running + jnp.log(jnp.where(present, summed, 1.0)), running))
    weighted = counts[0] * levels[0]
    for k in range(1, GRADES):
        weighted = weighted + counts[k] * levels[k]
    losses = (weighted - totals) / columns
    factors = []
    for h in range(GRADES):
        summed = counts[h] * jnp.exp(maxima[h] - levels[h])
        for k in range(h + 1, GRADES):
            summed = summed + counts[k] * jnp.exp(maxima[h] - levels[k])
        factors.append(summed)
    return stacked(maxima), stacked(factors + [losses])


GATHER = lax.GatherDimensionNumbers(
    offset_dims=(),
    collapsed_slice_dims=(0,),
    start_index_map=(0,),
    operand_batching_dims=(1,),
    start_indices_batching_dims=(1,),
)


def spread(table, grade):
    pieces = [
        lax.gather(
            table,
            grade[at : at + 8][..., None],
            GATHER,
            slice_sizes=(1, 1),
            mode=lax.GatherScatterMode.PROMISE_IN_BOUNDS,
        )
        for at in range(0, grade.shape[0], 8)
    ]
    return jnp.concatenate(pieces, axis=0)


def folded(op, block):
    return op(block.reshape(-1, 8, LANES), axis=0)


def kernel(
    q_hbm, c_hbm, w_hbm, g_hbm, loss_ref, out_ref,
    q_all, c_all, c_par, w_ref, w_t, g_in, g_t, es, sl, sl_par, z_rel, cnt, st_half, st, st_in, st_core, res,
    q_part, q_s1, q_r1, q_s2, q_r2, q_s3, q_r3,
    c_part, c_s1, c_r1, c_s2, c_r2, c_s3, c_rel, c_r3,
    send_sems, recv_sems, g_sems, in_sems,
):
    zh, x, y, zl, c = (lax.axis_index(a) for a in AXES)
    other = 1 - c
    wires = Wires(send_sems, recv_sems)
    send, arrive = wires.send, wires.arrive
    up_y, dn_y = {"y": (y + 1) % 4}, {"y": (y + 3) % 4}
    up_x, dn_x = {"x": (x + 1) % 4}, {"x": (x + 3) % 4}
    mate = {"c": other}
    zl2 = (zl + 2) % 4
    planes = (zl, zl + 1 - 2 * (zl % 2), zl2, 3 - zl)
    up_zh, dn_zh = (zh + zl // 2) % 2, (zh + 1 + zl // 2) % 2
    up_z, dn_z = {"zh": up_zh, "zl": zl2}, {"zh": dn_zh, "zl": zl2}

    def q_rows(core, k, dy, start=0, size=64):
        at = core * 1024 + planes[k] * 256 + (y + dy) % 4 * 64 + start
        return q_all.at[pl.ds(pl.multiple_of(at, 32), size), :]

    def c_rows(half, dx, start=0, size=128):
        at = half * 512 + (x + dx) % 4 * 128 + start
        return c_all.at[pl.ds(pl.multiple_of(at, 32), size), :]

    own = [
        pltpu.make_async_copy(q_hbm, q_rows(c, 0, 0), in_sems.at[0]),
        pltpu.make_async_copy(c_hbm, c_rows(zh, 0), in_sems.at[1]),
        pltpu.make_async_copy(w_hbm, w_ref, in_sems.at[2]),
    ]
    for copy in own:
        copy.start()

    def grade_copies(tile):
        core, plane, pair = tile // 8, tile // 2 % 4, tile % 2
        copies = []
        for i in range(2):
            at = (((pair * 2 + i) * 4 + plane) * 2 + core) * 64
            copies.append(
                pltpu.make_async_copy(
                    g_hbm.at[pl.ds(at, 64), :],
                    g_in.at[tile % 4, pl.ds(64 * i, 64), :],
                    g_sems.at[tile % 4, i],
                )
            )
        return copies

    for tile in range(4):
        for copy in grade_copies(tile):
            copy.start()

    barrier = pltpu.get_barrier_semaphore()
    greeted = [{"zl": planes[k]} for k in (1, 2, 3)] + [up_y, dn_y, up_x, dn_x, mate, {"zh": 1 - zh, "zl": zl2}]
    for device in greeted:
        pl.semaphore_signal(barrier, inc=1, device_id=device, device_id_type=pl.DeviceIdType.MESH)
    pl.semaphore_wait(barrier, len(greeted))

    for copy in own:
        copy.wait()
    q_own, c_own = q_rows(c, 0, 0), c_rows(zh, 0)
    for i in range(2):
        for h, where in ((0, up_z), (1, dn_z)):
            send(c_rows(zh, 0, 64 * h + 32 * i, 32), z_rel.at[h, pl.ds(32 * i, 32), :], ("zr", h, i), where)
    send(q_own, q_own, ("qy", 0, 0), up_y)
    send(q_own, q_own, ("qy", 0, 1), dn_y)
    send(c_own, c_own, ("cx", 0), up_x)
    send(c_own, c_own, ("cx", 1), dn_x)
    send(q_own, q_own, ("qz", 2), {"zl": planes[2]})
    send(q_own, q_own, ("qd", 0, 0), mate)
    for t in range(16):
        core, at = t // 8, t % 2 * 8 + t // 2 % 4
        pair = [w_ref[pl.ds(at, 1), :], w_ref[pl.ds(at + 4, 1), :]]
        pair[1 - core] = pltpu.roll(pair[1 - core], 64, 1)
        w_t[pl.ds(t, 1), :] = jnp.where(lax.broadcasted_iota(jnp.int32, (1, LANES), 1) < 64, *pair)

    def to_mate(k, dy):
        send(q_rows(c, k, dy), q_rows(c, k, dy), ("qd", k, dy), mate)

    def q_near(k):
        arrive(q_rows(c, k, 3), ("qy", k, 0), dn_y)
        send(q_rows(c, k, 3, 0, 32), q_rows(c, k, 3, 0, 32), ("qf", k, 0), up_y)
        to_mate(k, 3)
        arrive(q_rows(c, k, 1), ("qy", k, 1), up_y)
        send(q_rows(c, k, 1, 32, 32), q_rows(c, k, 1, 32, 32), ("qf", k, 1), dn_y)
        to_mate(k, 1)

    def q_far(k):
        arrive(q_rows(c, k, 2, 0, 32), ("qf", k, 0), dn_y)
        arrive(q_rows(c, k, 2, 32, 32), ("qf", k, 1), up_y)
        to_mate(k, 2)

    def q_over(k):
        arrive(q_rows(c, k, 0), ("qz", k), {"zl": planes[k if k < 3 else 1]})
        send(q_rows(c, k, 0), q_rows(c, k, 0), ("qy", k, 0), up_y)
        send(q_rows(c, k, 0), q_rows(c, k, 0), ("qy", k, 1), dn_y)
        if k == 2:
            send(q_rows(c, k, 0), q_rows(c, k, 0), ("qz", 3), {"zl": planes[1]})
        to_mate(k, 0)

    def c_near():
        arrive(c_rows(zh, 3), ("cx", 0), dn_x)
        send(c_rows(zh, 3, 0, 64), c_rows(zh, 3, 0, 64), ("cf", 0), up_x)
        arrive(c_rows(zh, 1), ("cx", 1), up_x)
        send(c_rows(zh, 1, 64, 64), c_rows(zh, 1, 64, 64), ("cf", 1), dn_x)

    def c_far():
        arrive(c_rows(zh, 2, 0, 64), ("cf", 0), dn_x)
        arrive(c_rows(zh, 2, 64, 64), ("cf", 1), up_x)

    def c_relay(i):
        for h, frm, where, there in ((0, dn_z, up_z, up_zh), (1, up_z, dn_z, dn_zh)):
            part = z_rel.at[h, pl.ds(32 * i, 32), :]
            arrive(part, ("zr", h, i), frm)
            send(part, c_rows(1 - there, 0, 64 * h + 32 * i, 32), ("cz", h, i), where)

    def q_leap():
        send(q_own, q_own, ("qz", 1), {"zl": planes[1]})

    def c_over(i):
        for h, frm in ((0, dn_z), (1, up_z)):
            part = c_rows(1 - zh, 0, 64 * h + 32 * i, 32)
            arrive(part, ("cz", h, i), frm)
            send(part, part, ("px", h, i, 0), up_x)
            send(part, part, ("px", h, i, 1), dn_x)

    def p_near(i):
        for h in range(2):
            below, above = c_rows(1 - zh, 3, 64 * h + 32 * i, 32), c_rows(1 - zh, 1, 64 * h + 32 * i, 32)
            arrive(below, ("px", h, i, 0), dn_x)
            if h == 0:
                send(below, below, ("pf", 0, i), up_x)
            arrive(above, ("px", h, i, 1), up_x)
            if h == 1:
                send(above, above, ("pf", 1, i), dn_x)

    def p_far():
        for i in range(2):
            for h, frm in ((0, dn_x), (1, up_x)):
                arrive(c_rows(1 - zh, 2, 64 * h + 32 * i, 32), ("pf", h, i), frm)

    def turn(tile):
        for copy in grade_copies(tile):
            copy.wait()
        for b in range(8):
            block = g_in[tile % 4, :, pl.ds(128 * b, 128)]
            g_t[pl.ds(128 * b, 128), pl.ds(128 * tile, 128)] = jnp.transpose(block)
        if tile + 4 < 16:
            for copy in grade_copies(tile + 4):
                copy.start()

        for h in range(2):

            def tally(i, held):
                at = pl.ds(pl.multiple_of(h * 512 + i * 64, 64), 64)
                grade = g_t[at, pl.ds(128 * tile, 128)]
                return tuple(v + folded(jnp.sum, jnp.where(grade == k, 1.0, 0.0)) for k, v in enumerate(held))

            held = lax.fori_loop(0, 8, tally, (jnp.zeros((8, LANES), F32),) * 4)
            held = [jnp.sum(v, axis=0, keepdims=True) for v in held]
            held.append(512.0 - (held[0] + held[1] + held[2] + held[3]))
            cnt[h, tile] = stacked(held)

    def pair_stats(half, first):
        lanes = [pl.ds(pl.multiple_of((first + i) * LANES, LANES), LANES) for i in range(2)]
        zero = jnp.zeros((8, LANES), F32)
        low = jnp.full((8, LANES), 32.0 * LOWEST, F32)

        def highest(n, held):
            at = pl.ds(pl.multiple_of(half * 512 + n * 64, 64), 64)
            new = []
            for i in range(2):
                score, grade = es[at, lanes[i]], g_t[at, lanes[i]]
                for k in range(GRADES):
                    found = folded(jnp.max, jnp.where(grade == k, score, 32.0 * LOWEST))
                    new.append(jnp.maximum(held[6 * i + k], found))
                new.append(held[6 * i + GRADES] + folded(jnp.sum, score))
            return tuple(new)

        held = lax.fori_loop(0, 8, highest, ((low,) * GRADES + (zero,)) * 2, unroll=2)
        maxima = [[jnp.max(v, axis=0, keepdims=True) for v in held[6 * i : 6 * i + GRADES]] for i in range(2)]
        total = [jnp.sum(held[6 * i + GRADES], axis=0, keepdims=True) * SCALE for i in range(2)]
        tables = [stacked(m) for m in maxima]

        def masses_of(n, held):
            at = pl.ds(pl.multiple_of(half * 512 + n * 64, 64), 64)
            new, values = [], []
            for i in range(2):
                score, grade = es[at, lanes[i]], g_t[at, lanes[i]]
                value = jnp.exp2((score - spread(tables[i], grade)) * EXP2_SCALE)
                values.append(value)
                for k in range(GRADES):
                    new.append(held[5 * i + k] + folded(jnp.sum, jnp.where(grade == k, value, 0.0)))
            for i in range(2):
                es[at, lanes[i]] = values[i]
            return tuple(new)

        held = lax.fori_loop(0, 8, masses_of, (zero,) * (2 * GRADES), unroll=2)
        for i in range(2):
            masses = [jnp.sum(v, axis=0, keepdims=True) for v in held[5 * i : 5 * i + GRADES]]
            counts = [cnt[half, first + i, pl.ds(k, 1), :] for k in range(GRADES)]
            st_half[half, first + i, pl.ds(0, 8), :] = stacked([m * SCALE for m in maxima[i]] + counts[:3])
            st_half[half, first + i, pl.ds(8, 8), :] = stacked(masses + counts[3:] + [total[i]])

    def unit(h, k):
        half = (zh + h) % 2
        cands = pl.ds(pl.multiple_of(half * 512, 512), 512)

        def one(core, _):
            n = core * 4 + planes[k]
            rows = pl.ds(pl.multiple_of(n * 256, 256), 256)
            es[cands, rows] = lax.dot_general(
                c_all[cands, :], q_all[rows, :], (((1,), (1,)), ((), ())), preferred_element_type=F32
            )
            pair_stats(half, 2 * n)
            return 0

        lax.fori_loop(0, 2, one, 0)

    columns = (y, y + 1 - 2 * (y % 2), (y + 2) % 4, 3 - y)
    slots = [(d, k) for k in range(4) for d in range(4)]

    def tile_of(d, k):
        return columns[d] // 2 * 8 + planes[k] * 2 + columns[d] % 2

    def chip(d, k):
        return {"y": columns[d], "zl": planes[k]}

    def st_out(k):
        for d in range(4):
            t, n = tile_of(d, k), k * 4 + d
            first, second = combine(
                [(st_half[h, t, pl.ds(0, 8), :], st_half[h, t, pl.ds(8, 8), :]) for h in range(2)]
            )
            st[n, pl.ds(0, 8), :] = first
            st[n, pl.ds(8, 8), :] = second
        for d in range(4):
            if (d, k) != (0, 0):
                n = k * 4 + d
                send(st.at[n], st_in.at[n], ("st", d, k), chip(d, k))

    def turns(first, last):
        for tile in range(first, last):
            turn(tile)

    def q_mate(k):
        for dy in range(4):
            arrive(q_rows(other, k, dy), ("qd", k, dy), mate)

    steps = [
        (turns, 0, 6), (q_near, 0), (c_relay, 0), (turns, 6, 8), (c_near,), (c_relay, 1), (q_leap,), (turns, 8, 11),
        (q_over, 2), (q_far, 0), (c_far,), (turns, 11, 13), (c_over, 0), (turns, 13, 16), (q_mate, 0), (c_over, 1),
        (unit, 0, 0), (q_near, 2), (p_near, 0), (q_over, 1), (p_near, 1), (q_over, 3), (q_far, 2), (q_mate, 2), (unit, 0, 2),
        (q_near, 1), (p_far,), (send, c_all, c_par, ("cp",), mate), (unit, 1, 0), (q_near, 3), (st_out, 0), (unit, 1, 2), (q_far, 1),
        (st_out, 2), (q_far, 3), (q_mate, 1), (unit, 0, 1), (unit, 1, 1), (st_out, 1), (q_mate, 3), (unit, 0, 3), (unit, 1, 3),
        (st_out, 3),
    ]
    for step, *given in steps:
        step(*given)

    mine = tile_of(0, 0)
    parts = [(st[0, pl.ds(0, 8), :], st[0, pl.ds(8, 8), :])]
    for d, k in slots[1:]:
        n = k * 4 + d
        arrive(st_in.at[n], ("st", d, k), chip(d, k))
        parts.append((st_in[n, pl.ds(0, 8), :], st_in[n, pl.ds(8, 8), :]))
    first, second = combine(parts)
    st_core[0, pl.ds(0, 8), :] = first
    st_core[0, pl.ds(8, 8), :] = second
    send(st_core.at[0], st_core.at[1], ("sd",), mate)
    arrive(st_core.at[1], ("sd",), mate)
    first, second = combine([(first, second), (st_core[1, pl.ds(0, 8), :], st_core[1, pl.ds(8, 8), :])])
    first, second = outcome(first, second, 32768.0)
    res[mine, pl.ds(0, 8), :] = first
    res[mine, pl.ds(8, 8), :] = second
    for d, k in reversed(slots[1:]):
        send(res.at[mine], res.at[mine], ("sr", d, k), chip(d, k))
    arrive(c_par, ("cp",), mate)
    for d, k in slots[1:]:
        arrive(res.at[tile_of(d, k)], ("sr", d, k), chip(d, k))
    def losses_out():
        found = [res[t, pl.ds(13, 1), :] for t in range(16)]
        low_lanes = lax.broadcasted_iota(jnp.int32, (1, LANES), 1) < 64
        for v in range(4):
            for p in range(4):
                pair = [found[core * 8 + p * 2 + v // 2] for core in range(2)]
                pair[1 - v % 2] = pltpu.roll(pair[1 - v % 2], 64, 1)
                loss_ref[pl.ds(v * 4 + p, 1), :] = jnp.where(low_lanes, pair[0], pair[1])
        loss_ref[pl.ds(16, 8), :] = jnp.zeros((8, LANES), F32)

    row = lax.broadcasted_iota(jnp.int32, (8, LANES), 0)
    for t in range(16):
        weight = w_t[pl.ds(t, 1), :] * SCALE
        for h in range(2):
            table = res[t, pl.ds(8, 8), :] * jnp.exp(st_half[h, t, pl.ds(0, 8), :] - res[t, pl.ds(0, 8), :])
            table = jnp.where(row < GRADES, table, 0.0) * weight
            st_half[h, t, pl.ds(8, 8), :] = jnp.where(row == 7, weight, table)

    def slope_block(j, d):
        half = (zh + 1 - j) % 2
        at = pl.ds(pl.multiple_of(half * 512 + (x + d) % 4 * 128, 128), 128)

        def one(t, _):
            lanes = pl.ds(pl.multiple_of(t * LANES, LANES), LANES)
            table = st_half[half, t, pl.ds(8, 8), :]
            sl[at, lanes] = (spread(table, g_t[at, lanes]) * es[at, lanes] - table[7:8]).astype(BF)
            return 0

        lax.fori_loop(0, 16, one, 0, unroll=2)

    def slopes_out(j):
        cands = pl.ds(pl.multiple_of((zh + 1 - j) % 2 * 512, 512), 512)
        send(sl.at[cands, pl.ds(pl.multiple_of(other * 1024, 1024), 1024)], sl_par.at[cands, :], ("sl", j), mate)

    def lanes_of(core, plane):
        return pl.ds(pl.multiple_of(core * 1024 + plane * 256, 256), 256)

    def slopes_mate(j):
        cands = pl.ds(pl.multiple_of((zh + 1 - j) % 2 * 512, 512), 512)
        arrive(sl_par.at[cands, :], ("sl", j), mate)

    def c_block(d, start=0, size=128):
        return pl.ds(pl.multiple_of((x + d) % 4 * 128 + start, 32), size)

    def c_dot(j, d):
        at = pl.multiple_of((zh + 1 - j) % 2 * 512 + (x + d) % 4 * 128, 128)
        c_part[j, c_block(d), :] = jnp.dot(sl[pl.ds(at, 128), :], q_all[...], preferred_element_type=F32)

    def c_far_part(j):
        c_dot(j, 2)
        for side in range(2):
            c_s1[j, side] = c_part[j, c_block(2, 64 * side, 64), :].astype(BF)
        for i in range(2):
            for side, where in ((0, up_x), (1, dn_x)):
                at = pl.ds(32 * i, 32)
                send(c_s1.at[j, side, at, :], c_r1.at[j, side, at, :], ("s1", j, side, i), where)

    def c_rest(j):
        for d, side in ((1, 0), (3, 1)):
            c_dot(j, d)
            at = pl.ds(64 - 64 * side, 64)
            c_s2[j, side, at, :] = c_part[j, c_block(d, 64 - 64 * side, 64), :].astype(BF)
        for i in range(2):
            for side, where in ((0, up_x), (1, dn_x)):
                at = pl.ds(64 - 64 * side + 32 * i, 32)
                send(c_s2.at[j, side, at, :], c_r2.at[j, side, at, :], ("s2", j, side, i), where)

    def c_mid(j, i):
        for d, side, frm, where in ((1, 0, dn_x, up_x), (3, 1, up_x, dn_x)):
            half = pl.ds(32 * i, 32)
            arrive(c_r1.at[j, side, half, :], ("s1", j, side, i), frm)
            at = pl.ds(64 * side + 32 * i, 32)
            own_part = c_part[j, c_block(d, 64 * side + 32 * i, 32), :]
            c_s2[j, side, at, :] = (own_part + c_r1[j, side, half, :].astype(F32)).astype(BF)
            send(c_s2.at[j, side, at, :], c_r2.at[j, side, at, :], ("s4", j, side, i), where)

    def c_take(j, i):
        for side, frm in ((0, dn_x), (1, up_x)):
            arrive(c_r2.at[j, side, pl.ds(64 - 64 * side + 32 * i, 32), :], ("s2", j, side, i), frm)
            arrive(c_r2.at[j, side, pl.ds(64 * side + 32 * i, 32), :], ("s4", j, side, i), frm)

    def c_leave(i):
        c_take(0, i)
        for h, where in ((0, up_z), (1, dn_z)):
            at = pl.ds(64 * h + 32 * i, 32)
            total = c_part[0, c_block(0, 64 * h + 32 * i, 32), :] + c_r2[0, 0, at, :].astype(F32) + c_r2[0, 1, at, :].astype(F32)
            c_s3[at, :] = total.astype(BF)
            send(c_s3.at[at, :], c_rel.at[h, pl.ds(32 * i, 32), :], ("t1", h, i), where)

    def c_pass(i):
        for h, frm, where in ((0, dn_z, up_z), (1, up_z, dn_z)):
            part = c_rel.at[h, pl.ds(32 * i, 32), :]
            arrive(part, ("t1", h, i), frm)
            send(part, c_r3.at[pl.ds(64 * h + 32 * i, 32), :], ("t2", h, i), where)

    def c_end():
        for i in range(2):
            c_take(1, i)
        total = c_part[1, c_block(0), :] + c_r2[1, 0].astype(F32) + c_r2[1, 1].astype(F32)
        for i in range(2):
            for h, frm in ((0, dn_z), (1, up_z)):
                arrive(c_r3.at[pl.ds(64 * h + 32 * i, 32), :], ("t2", h, i), frm)
        out_ref[pl.ds(64, 128), :] = total + c_r3[...].astype(F32)

    dims = (((0,), (0,)), ((), ()))

    def q_block(d, start, size):
        return pl.ds(pl.multiple_of((y + d) % 4 * 64 + start, 32), size)

    def q_dot(k):
        plane = planes[k]
        q_part[k] = lax.dot_general(
            sl[:, lanes_of(c, plane)], c_all[...], dims, preferred_element_type=F32
        ) + lax.dot_general(sl_par[:, lanes_of(0, plane)], c_par[...], dims, preferred_element_type=F32)

        q_s1[k, 0] = q_part[k, q_block(2, 0, 32), :].astype(BF)
        q_s1[k, 1] = q_part[k, q_block(2, 32, 32), :].astype(BF)
        send(q_s1.at[k, 0], q_r1.at[k, 0], ("r1", k, 0), up_y)
        send(q_s1.at[k, 1], q_r1.at[k, 1], ("r1", k, 1), dn_y)
        for d, side, where in ((1, 0, up_y), (3, 1, dn_y)):
            at = pl.ds(32 - 32 * side, 32)
            q_s2[k, side, at, :] = q_part[k, q_block(d, 32 - 32 * side, 32), :].astype(BF)
            send(q_s2.at[k, side, at, :], q_r2.at[k, side, at, :], ("r2", k, side), where)

    def q_mid(k):
        for d, side, frm, where in ((1, 0, dn_y, up_y), (3, 1, up_y, dn_y)):
            arrive(q_r1.at[k, side], ("r1", k, side), frm)
            at = pl.ds(32 * side, 32)
            q_s2[k, side, at, :] = (q_part[k, q_block(d, 32 * side, 32), :] + q_r1[k, side].astype(F32)).astype(BF)
            send(q_s2.at[k, side, at, :], q_r2.at[k, side, at, :], ("r4", k, side), where)

    def q_sum(k):
        for side, frm in ((0, dn_y), (1, up_y)):
            arrive(q_r2.at[k, side, pl.ds(32 - 32 * side, 32), :], ("r2", k, side), frm)
            arrive(q_r2.at[k, side, pl.ds(32 * side, 32), :], ("r4", k, side), frm)
        at = pl.ds(pl.multiple_of(y * 64, 64), 64)
        return q_part[k, at, :] + q_r2[k, 0].astype(F32) + q_r2[k, 1].astype(F32)

    def q_leave(k):
        total = q_sum(k)
        if k == 2:
            arrive(q_r3.at[2], ("r3", 3), {"zl": planes[1]})
            total = total + q_r3[2].astype(F32)
        q_s3[k - 1] = total.astype(BF)
        send(q_s3.at[k - 1], q_r3.at[k - 1], ("r3", k), {"zl": planes[k if k < 3 else 1]})

    def q_end():
        total = q_sum(0)
        for k in (1, 2):
            arrive(q_r3.at[k - 1], ("r3", k), {"zl": planes[k]})
            total = total + q_r3[k - 1].astype(F32)
        out_ref[pl.ds(0, 64), :] = total

    steps = [
        (slope_block, 0, 2), (c_far_part, 0), (slope_block, 0, 1), (slope_block, 0, 3), (c_rest, 0), (slope_block, 0, 0),
        (slopes_out, 0), (c_mid, 0, 0), (slope_block, 1, 0), (slope_block, 1, 1), (slope_block, 1, 2), (slope_block, 1, 3),
        (slopes_out, 1), (c_mid, 0, 1), (c_dot, 0, 0), (slopes_mate, 0), (slopes_mate, 1), (q_dot, 3), (c_leave, 0), (q_dot, 2),
        (q_mid, 3), (c_leave, 1), (q_dot, 1), (c_pass, 0), (q_mid, 2), (q_leave, 3), (q_dot, 0), (c_pass, 1), (q_mid, 1),
        (c_far_part, 1), (c_rest, 1), (q_leave, 1), (q_leave, 2), (c_mid, 1, 0), (c_mid, 1, 1), (c_dot, 1, 0), (q_mid, 0),
        (losses_out,), (q_end,), (c_end,),
    ]
    for step, *given in steps:
        step(*given)
    wires.finish()


def local(queries, candidates, grades, query_weights):
    vmem = pl.BlockSpec(memory_space=pltpu.VMEM)
    weights = query_weights.reshape(16, LANES)
    shapes = [
        ((2048, 1024), BF), ((1024, 1024), BF), ((1024, 1024), BF), ((16, LANES), F32), ((16, LANES), F32), ((4, 128, 1024), jnp.int32),
        ((1024, 2048), jnp.int32), ((1024, 2048), F32), ((1024, 2048), BF), ((1024, 1024), BF),
        ((2, 64, 1024), BF), ((2, 16, 8, LANES), F32), ((2, 16, 16, LANES), F32), ((16, 16, LANES), F32),
        ((16, 16, LANES), F32), ((2, 16, LANES), F32), ((16, 16, LANES), F32),
        ((4, 256, 1024), F32), ((4, 2, 32, 1024), BF), ((4, 2, 32, 1024), BF), ((4, 2, 64, 1024), BF),
        ((4, 2, 64, 1024), BF), ((3, 64, 1024), BF), ((3, 64, 1024), BF),
        ((2, 512, 1024), F32), ((2, 2, 64, 1024), BF), ((2, 2, 64, 1024), BF), ((2, 2, 128, 1024), BF),
        ((2, 2, 128, 1024), BF), ((128, 1024), BF), ((2, 64, 1024), BF), ((128, 1024), BF),
    ]
    losses, out = pl.pallas_call(
        kernel,
        out_shape=(jax.ShapeDtypeStruct((24, LANES), F32), jax.ShapeDtypeStruct((192, 1024), F32)),
        in_specs=[pl.BlockSpec(memory_space=pl.ANY)] * 4,
        out_specs=(vmem, vmem),
        scratch_shapes=[pltpu.VMEM(shape, dtype) for shape, dtype in shapes]
        + [
            pltpu.SemaphoreType.DMA((192,)),
            pltpu.SemaphoreType.DMA((192,)),
            pltpu.SemaphoreType.DMA((4, 2)),
            pltpu.SemaphoreType.DMA((3,)),
        ],
        compiler_params=pltpu.CompilerParams(
            collective_id=0, has_side_effects=True, vmem_limit_bytes=66 * 1000 * 1000
        ),
        name="listmle",
    )(queries, candidates, weights, grades)
    return losses[:16].reshape(2048), out[:64].astype(BF), out[64:].astype(BF)


def solution(mesh):
    split = Mesh(mesh.devices.reshape(2, 4, 4, 4, 2), AXES)
    return jax.shard_map(
        local,
        mesh=split,
        in_specs=(P(AXES_Q := ROWS + COL, None), P(COL + ROWS, None), P(ROWS, COL), P(ROWS)),
        out_specs=(P(ROWS), P(AXES_Q, None), P(COL + ROWS, None)),
        check_vma=False,
    )
```
